128 devices in a mesh: tp: 128 (over z, y, x, core).
Axes of the slice: x: 4, y: 4, z: 4, core: 2. Of those that a mesh axis runs over, the one named last changes fastest.
Arguments:
- tok_ids: int32 [2, 128], replicated
- next_ids: int32 [2, 128], replicated
- seq_lens: int32 [128], replicated
- embed: bfloat16 [256000, 2048], P('tp')
- ln_gain: bfloat16 [2048], replicated
- w_in: bfloat16 [2048, 35328], P(None, 'tp')
- w_out: bfloat16 [18432, 2048], P('tp')
- final_gain: bfloat16 [2048], replicated
- k_cache: bfloat16 [128, 1024, 256], P('tp')
- v_cache: bfloat16 [128, 1024, 256], P('tp')
Outputs:
- output 1: float32 [2, 128], replicated
- output 2: bfloat16 [128, 1024, 256], P('tp')
- output 3: bfloat16 [128, 1024, 256], P('tp')
All inputs are finite; a program needn't handle non-finite values.
Results may differ from the reference program's by a relative error of at most 0.001.
Values are sent between devices in bfloat16 or wider.
A program may use at most 1 GiB of HBM per device.

```python
import jax
import jax.numpy as jnp
from jax import lax

D = 2048
HEADS = 8
HEAD = 256
FF = 16384
VOCAB = 256000
GROUP = 128
BATCH_DEV = 1
CACHE_LEN = 1024
NUM_STEPS = 2

BATCH = BATCH_DEV * GROUP
QKV_WIDTH = (HEADS + 2) * HEAD
ATTN_WIDTH = HEADS * HEAD
QKV_DEV = QKV_WIDTH // GROUP
ATTN_DEV = ATTN_WIDTH // GROUP
FF_DEV = FF // GROUP
IN_DEV = QKV_DEV + 2 * FF_DEV
OUT_DEV = ATTN_DEV + FF_DEV
IN_WIDTH = IN_DEV * GROUP
OUT_WIDTH = OUT_DEV * GROUP
MAP_ROWS = min(BATCH, 64)
MAP_COUNT = BATCH // MAP_ROWS
NORM_EPS = 1e-6
ROPE_BASE = 10000.0


def setup_inputs(seed: int = 0) -> dict:
    key_list = jax.random.split(jax.random.key(seed), 11)
    tok_ids = jax.random.randint(key_list[0], (NUM_STEPS, BATCH), 0, VOCAB, dtype=jnp.int32)
    next_ids = jax.random.randint(key_list[1], (NUM_STEPS, BATCH), 0, VOCAB, dtype=jnp.int32)
    base_lens = jax.random.randint(key_list[2], (BATCH,), 0, CACHE_LEN - 1, dtype=jnp.int32)
    perm_order = jax.random.permutation(key_list[3], BATCH)
    seq_lens = base_lens.at[perm_order[0]].set(CACHE_LEN - 2).at[perm_order[1]].set(0)
    embed = jax.random.normal(key_list[4], (VOCAB, D), jnp.float32).astype(jnp.bfloat16)
    ln_gain = (1.0 + 0.3 * jax.random.normal(key_list[5], (D,), jnp.float32)).astype(jnp.bfloat16)
    w_in = (jax.random.normal(key_list[6], (D, IN_WIDTH), jnp.float32) * D ** -0.5).astype(jnp.bfloat16)
    row_scale = jnp.where(jnp.arange(OUT_WIDTH) % OUT_DEV < ATTN_DEV, 2.0 * ATTN_WIDTH ** -0.5, FF ** -0.5)
    w_out = (jax.random.normal(key_list[7], (OUT_WIDTH, D), jnp.float32) * row_scale[:, None]).astype(jnp.bfloat16)
    final_gain = (1.6 * (1.0 + 0.3 * jax.random.normal(key_list[8], (D,), jnp.float32))).astype(jnp.bfloat16)
    k_cache = jax.random.normal(key_list[9], (BATCH, CACHE_LEN, HEAD), jnp.float32).astype(jnp.bfloat16)
    v_cache = jax.random.normal(key_list[10], (BATCH, CACHE_LEN, HEAD), jnp.float32).astype(jnp.bfloat16)
    return {'tok_ids': tok_ids, 'next_ids': next_ids, 'seq_lens': seq_lens, 'embed': embed, 'ln_gain': ln_gain, 'w_in': w_in, 'w_out': w_out, 'final_gain': final_gain, 'k_cache': k_cache, 'v_cache': v_cache}


def layer_norm(values, gain_vec):
    centered = values.astype(jnp.float32)
    centered = centered - jnp.mean(centered, axis=-1, keepdims=True)
    variance = jnp.mean(jnp.square(centered), axis=-1, keepdims=True)
    scaled = centered * lax.rsqrt(variance + NORM_EPS) * gain_vec.astype(jnp.float32)
    return scaled.astype(jnp.bfloat16)


def rotary(vectors, positions):
    half_dim = vectors.shape[-1] // 2
    inv_freq = ROPE_BASE ** (-jnp.arange(half_dim, dtype=jnp.float32) / half_dim)
    angles = positions.astype(jnp.float32)[..., None] * inv_freq
    cosine = jnp.cos(angles)
    sine_val = jnp.sin(angles)
    first_half = vectors[..., :half_dim]
    second_half = vectors[..., half_dim:]
    return jnp.concatenate([first_half * cosine - second_half * sine_val, second_half * cosine + first_half * sine_val], axis=-1)


def block_steps(tok_blk, next_blk, len_blk, k_blk, v_blk, embed, ln_gain, w_in, w_out, final_gain):
    row_count = len_blk.shape[0]
    time_ids = jnp.arange(CACHE_LEN)
    step_logp = []
    for step_idx in range(NUM_STEPS):
        positions = len_blk + step_idx
        x_rows = embed[tok_blk[step_idx]]
        normed = layer_norm(x_rows, ln_gain)
        proj_out = jnp.dot(normed, w_in, preferred_element_type=jnp.float32).astype(jnp.bfloat16)
        proj_out = proj_out.reshape(row_count, GROUP, IN_DEV)
        qkv_vec = proj_out[:, :, :QKV_DEV].reshape(row_count, QKV_WIDTH)
        gate_proj = proj_out[:, :, QKV_DEV:QKV_DEV + FF_DEV].astype(jnp.float32)
        up_proj = proj_out[:, :, QKV_DEV + FF_DEV:].astype(jnp.float32)
        mlp_act = (jax.nn.silu(gate_proj) * up_proj).astype(jnp.bfloat16)
        queries = qkv_vec[:, :ATTN_WIDTH].reshape(row_count, HEADS, HEAD).astype(jnp.float32)
        q_rot = (rotary(queries, positions[:, None]) * HEAD ** -0.5).astype(jnp.bfloat16)
        k_new = rotary(qkv_vec[:, ATTN_WIDTH:ATTN_WIDTH + HEAD].astype(jnp.float32), positions).astype(jnp.bfloat16)
        v_new = qkv_vec[:, ATTN_WIDTH + HEAD:]
        write_mask = time_ids[None, :, None] == positions[:, None, None]
        k_blk = jnp.where(write_mask, k_new[:, None, :], k_blk)
        v_blk = jnp.where(write_mask, v_new[:, None, :], v_blk)
        scores = jnp.einsum('bhd,btd->bht', q_rot.astype(jnp.float32), k_blk.astype(jnp.float32))
        visible = time_ids[None, None, :] <= positions[:, None, None]
        attn_probs = jax.nn.softmax(jnp.where(visible, scores, -jnp.inf), axis=-1).astype(jnp.bfloat16)
        attn_out = jnp.einsum('bht,btd->bhd', attn_probs.astype(jnp.float32), v_blk.astype(jnp.float32)).astype(jnp.bfloat16)
        attn_grp = attn_out.reshape(row_count, GROUP, ATTN_DEV)
        combined = jnp.concatenate([attn_grp, mlp_act], axis=2).reshape(row_count, OUT_WIDTH)
        layer_out = jnp.dot(combined, w_out, preferred_element_type=jnp.float32).astype(jnp.bfloat16)
        resid_sum = x_rows.astype(jnp.float32) + layer_out.astype(jnp.float32)
        final_normed = layer_norm(resid_sum, final_gain)
        logits = jnp.dot(final_normed, embed.T, preferred_element_type=jnp.float32) * D ** -0.5
        picked = jnp.take_along_axis(logits, next_blk[step_idx][:, None], axis=1)[:, 0]
        step_logp.append(picked - jax.nn.logsumexp(logits, axis=1))
    return jnp.stack(step_logp), k_blk, v_blk


def reference(tok_ids, next_ids, seq_lens, embed, ln_gain, w_in, w_out, final_gain, k_cache, v_cache):
    tok_grp = tok_ids.reshape(NUM_STEPS, MAP_COUNT, MAP_ROWS).transpose(1, 0, 2)
    next_grp = next_ids.reshape(NUM_STEPS, MAP_COUNT, MAP_ROWS).transpose(1, 0, 2)
    len_grp = seq_lens.reshape(MAP_COUNT, MAP_ROWS)
    k_grp = k_cache.reshape(MAP_COUNT, MAP_ROWS, CACHE_LEN, HEAD)
    v_grp = v_cache.reshape(MAP_COUNT, MAP_ROWS, CACHE_LEN, HEAD)

    def run_group(group_in):
        return block_steps(group_in[0], group_in[1], group_in[2], group_in[3], group_in[4], embed, ln_gain, w_in, w_out, final_gain)

    logp_grp, k_done, v_done = lax.map(run_group, (tok_grp, next_grp, len_grp, k_grp, v_grp))
    log_probs = logp_grp.transpose(1, 0, 2).reshape(NUM_STEPS, BATCH)
    return log_probs, k_done.reshape(BATCH, CACHE_LEN, HEAD), v_done.reshape(BATCH, CACHE_LEN, HEAD)
```

```python
import jax
import jax.numpy as jnp
from jax import lax
from jax.experimental import pallas as pl
from jax.experimental.pallas import tpu as pltpu
from jax.sharding import PartitionSpec as P

ROPE_BASE = 10000.0
NORM_EPS = 1e-6
F32 = jnp.float32
BF16 = jnp.bfloat16
MESH = pl.DeviceIdType.MESH

D = 2048
VDEV = 2000
VPAD = 2048
HEADS = 8
HEAD = 256
CACHE = 1024
TILES = D // 128
QKV_DEV = 20
ATT_DEV = 16
LANE = 128
WIDE = 256
ROWS = 32
SIDE = 16
LINE = 4
SUB = 8
FOLD = 512
LINE_ORDER = (2, 1, 3)


def rem(value, size):
    return lax.rem(value, jnp.int32(size))


def div(value, size):
    return lax.div(value, jnp.int32(size))


def iota(shape, dim):
    return lax.broadcasted_iota(jnp.int32, shape, dim)


def nt_dot(left, right):
    return lax.dot_general(left, right, (((1,), (1,)), ((), ())), preferred_element_type=F32)


def nn_dot(left, right):
    return lax.dot_general(left, right, (((1,), (0,)), ((), ())), preferred_element_type=F32)


def device_of(core, line, plane):
    return div(plane, LINE) * ROWS + rem(plane, LINE) * (SUB - 6 * core) + line * (2 + 6 * core) + core


def kernel(tok_ref, next_ref, lens_ref, emb_hbm, lng_ref, win_hbm, wout_hbm, fing_ref, k_hbm, v_hbm, freq_ref,
           logp_ref, kout_hbm, vout_hbm,
           emb, win, wgu, wout, kbuf, vbuf, wq, wext, sel, hot,
           send_d, own, recv_d, send_f, recv_f, acc, fold32, afold, fold16, recv_p, x_own, gains,
           ag, unf, lhs, qlhs, qmsg, recv_q, qrows, qkrow, afbuf, amsg, recv_a, alhs, mlp, lg,
           fin_s, fin_p, fin_f, fin_d,
           ld, sd_s, sd_r, sf_s, sf_r, sp_s, sp_r, ap_s, ap_r, af_s, af_r, ad_s, ad_r,
           wd_s, wd_r, wf_s, wf_r, q_s, q_r, a_s, a_r, fp_s, fp_r, ff_s, ff_r, fd_s, fd_r):
    me = lax.axis_index('tp')
    core = rem(me, 2)
    other = 1 - core
    zc, yc, xc = div(me, ROWS), rem(div(me, SUB), LINE), rem(div(me, 2), LINE)
    line = xc * other + yc * core
    line_o = yc * other + xc * core
    plane = zc * LINE + yc * other + xc * core
    partner = me + 1 - 2 * core
    me_slot = rem(me, ROWS)
    partner_slot = rem(partner, ROWS)

    def line_dev(k):
        return device_of(core, rem(line + k, LINE), plane)

    def plane_dev(pp):
        return device_of(core, line, pp)

    def rcopy(src, dst, ss, rs, dev):
        return pltpu.make_async_remote_copy(src_ref=src, dst_ref=dst, send_sem=ss, recv_sem=rs, device_id=(dev,), device_id_type=MESH)

    def local_copies():
        out = []
        for n in range(SUB):
            cols = pl.ds(n * WIDE, WIDE)
            out.append(pltpu.make_async_copy(emb_hbm.at[:, cols], emb.at[pl.ds(0, VDEV), cols], ld.at[n]))
        out.append(pltpu.make_async_copy(win_hbm, win, ld.at[SUB]))
        out.append(pltpu.make_async_copy(wout_hbm, wout, ld.at[9]))
        out.append(pltpu.make_async_copy(k_hbm.at[0], kbuf, ld.at[10]))
        out.append(pltpu.make_async_copy(v_hbm.at[0], vbuf, ld.at[11]))
        return out

    loads = local_copies()
    for copy in loads:
        copy.start()

    wext[...] = jnp.zeros_like(wext)

    barrier = pltpu.get_barrier_semaphore()
    pl.semaphore_signal(barrier, inc=1, device_id=(partner,), device_id_type=MESH)
    for k in range(1, LINE):
        pl.semaphore_signal(barrier, inc=1, device_id=(line_dev(k),), device_id_type=MESH)

    def greet(k, carry):
        pl.semaphore_signal(barrier, inc=1, device_id=(plane_dev(rem(plane + k, SIDE)),), device_id_type=MESH)
        return carry

    lax.fori_loop(1, SIDE, greet, 0)

    emb[pl.ds(VDEV, VPAD - VDEV), :] = jnp.zeros((VPAD - VDEV, D), BF16)
    for t in range(TILES):
        gains[pl.ds(t, 1), :] = lng_ref[:, t * LANE:(t + 1) * LANE].astype(F32)
        gains[pl.ds(TILES + t, 1), :] = fing_ref[:, t * LANE:(t + 1) * LANE].astype(F32)

    row = iota((WIDE, LANE), 0)
    lane = iota((WIDE, LANE), 1)
    half = row >> 7
    row_core = core + (1 - half) * (1 - 2 * core)
    row_p = (row >> 1) & 15
    row_b = (row_p >> 2) * ROWS + (row_p & 3) * (SUB - 6 * row_core) + ((row >> 5) & 3) * (2 + 6 * row_core) + row_core
    tok_val = jnp.where((row & 1) == 0, tok_ref[0:1, :], tok_ref[1:2, :]).astype(F32)
    tok_col = jnp.sum(jnp.where(lane == row_b, tok_val, 0.0), axis=1, keepdims=True)
    local_col = tok_col.astype(jnp.int32) - me * VDEV
    for t in range(VPAD // LANE):
        hot[:, t * LANE:(t + 1) * LANE] = jnp.where(lane + t * LANE == local_col, 1.0, 0.0).astype(BF16)

    pl.semaphore_wait(barrier, 19)

    for n in range(SUB):
        cols = pl.ds(n * WIDE, WIDE)
        loads[n].wait()
        part = nn_dot(hot[...], emb[:, cols])
        send_d[0, :, cols] = part[0:LANE].astype(BF16)
        own[:, cols] = part[LANE:WIDE]

    def d_copy(r, k):
        src = pl.ds(pl.multiple_of(rem(line_o + k, LINE) * ROWS, ROWS), ROWS)
        return rcopy(send_d.at[r, src], recv_d.at[r, k], sd_s.at[r, k], sd_r.at[r, k], partner)

    def f_copy(r, k):
        return rcopy(send_f.at[r, k], recv_f.at[r, k], sf_s.at[r, k], sf_r.at[r, k], line_dev(k))

    def scatter_line(r):
        for k in LINE_ORDER + (0,):
            d_copy(r, k).start()
        for k in LINE_ORDER + (0,):
            d_copy(r, k).wait_recv()
            chunk = pl.ds(pl.multiple_of(rem(line + k, LINE) * ROWS, ROWS), ROWS)
            total = own[chunk, :] + recv_d[r, k].astype(F32)
            if k:
                send_f[r, k] = total.astype(BF16)
                f_copy(r, k).start()
            else:
                acc[...] = total

    def scatter_line_end(r):
        for k in (1, 3, 2):
            f_copy(r, k).wait_recv()
            acc[...] += recv_f[r, k].astype(F32)
        for t in range(TILES):
            fold32[pl.ds(t, ROWS, stride=TILES), :] = acc[:, t * LANE:(t + 1) * LANE]

    def each_plane(fn):
        def body(k, carry):
            fn(k)
            return carry
        lax.fori_loop(1, SIDE, body, 0)

    def ahead(k):
        return rem(plane + k, SIDE)

    def behind(k):
        return rem(plane + SIDE - k, SIDE)

    def p_rows(pp):
        return pl.ds(pl.multiple_of(pp * ROWS, ROWS), ROWS)

    def p_copy(r, k, slot):
        return rcopy(fold16.at[r, p_rows(ahead(k))], recv_p.at[r, slot], sp_s.at[r, k], sp_r.at[r, k], plane_dev(ahead(k)))

    def scatter_plane(r):
        each_plane(lambda k: p_copy(r, k, plane).start())

    def scatter_plane_end(r):
        each_plane(lambda k: p_copy(r, k, behind(k)).wait_recv())

        def add(k, total):
            return total + recv_p[r, behind(k)].astype(F32)
        return lax.fori_loop(1, SIDE, add, fold32[p_rows(plane), :])

    def norm_rows(values, gain):
        out = []
        for s in range(2):
            v = values[s * TILES:(s + 1) * TILES]
            v = v - jnp.sum(v, axis=(0, 1), keepdims=True) * (1.0 / D)
            var = jnp.sum(v * v, axis=(0, 1), keepdims=True) * (1.0 / D)
            out.append(v * lax.rsqrt(var + NORM_EPS) * gain)
        return jnp.concatenate(out, axis=0).astype(BF16)

    def ap_copy(r, k, slot):
        ref = ag.at[r, core, line, p_rows(slot)]
        return rcopy(ref, ref, ap_s.at[r, k], ap_r.at[r, k], plane_dev(ahead(k)))

    def al_copy(r, k, slot):
        ref = ag.at[r, core, slot]
        return rcopy(ref, ref, af_s.at[r, k], af_r.at[r, k], line_dev(k))

    def ad_copy(r, k, side, slot):
        ref = ag.at[r, side, slot]
        return rcopy(ref, ref, ad_s.at[r, k], ad_r.at[r, k], partner)

    def gather_plane(r, rows):
        ag[r, core, line, p_rows(plane), :] = rows
        each_plane(lambda k: ap_copy(r, k, plane).start())
        each_plane(lambda k: ap_copy(r, k, behind(k)).wait_recv())
        for k in LINE_ORDER:
            al_copy(r, k, line).start()
        ad_copy(r, 0, core, line).start()

    def gather_line(r):
        for k in (1, 3, 2):
            back = rem(line + LINE - k, LINE)
            al_copy(r, k, back).wait_recv()
            ad_copy(r, k, core, back).start()

    def gather_end(r):
        for k in (0, 1, 3, 2):
            ad_copy(r, k, other, rem(line_o + LINE - k, LINE)).wait_recv()

    def unfold(r, sides):
        for h in range(2):
            for q in range(LINE):
                base = (h * LINE + q) * FOLD
                unf[pl.ds(base, FOLD), :] = ag[r, sides[h], q].astype(F32)
        for t in range(TILES):
            lhs[:, t * LANE:(t + 1) * LANE] = unf[pl.ds(t, WIDE, stride=TILES), :].astype(BF16)

    scatter_line(0)

    loads[SUB].wait()
    loads[9].wait()

    def wq_rows(slot, count):
        return pl.ds(pl.multiple_of(slot * ROWS, ROWS), count * ROWS)

    wq[wq_rows(line * 2 + core, 1), :] = win[0:ROWS, :]
    wext[me_slot] = wout[0:ATT_DEV, :]

    def wd_copies():
        return (rcopy(wq.at[wq_rows(line * 2 + core, 1)], wq.at[wq_rows(line_o * 2 + core, 1)], wd_s.at[0], wd_r.at[0], partner),
                rcopy(wext.at[me_slot], wext.at[me_slot], wd_s.at[1], wd_r.at[1], partner))

    for copy in wd_copies():
        copy.start()

    def wf_copies(k, line_slot, pair_slot):
        q_ref = wq.at[wq_rows(line_slot * 2, 2)]
        e_ref = wext.at[pl.ds(pair_slot, 2)]
        return (rcopy(q_ref, q_ref, wf_s.at[0, k], wf_r.at[0, k], line_dev(k)),
                rcopy(e_ref, e_ref, wf_s.at[1, k], wf_r.at[1, k], line_dev(k)))

    my_pair = me_slot - core

    def pair_of(k):
        return my_pair + (rem(line + LINE - k, LINE) - line) * (2 + 6 * core)

    rcopy(wq.at[wq_rows(line * 2 + core, 1)], wq.at[wq_rows(line * 2 + other, 1)], wd_s.at[0], wd_r.at[0], partner).wait_recv()
    rcopy(wext.at[me_slot], wext.at[partner_slot], wd_s.at[1], wd_r.at[1], partner).wait_recv()
    for k in LINE_ORDER:
        for copy in wf_copies(k, line, my_pair):
            copy.start()

    scatter_line_end(0)
    fold16[0] = fold32[...].astype(BF16)
    scatter_plane(0)

    for t in range(TILES):
        wgu[:, t * LANE:(t + 1) * LANE] = win[QKV_DEV:QKV_DEV + WIDE, t * LANE:(t + 1) * LANE]

    def column_ids(hh):
        col = iota((1, HEAD), 1) + hh * HEAD
        src = (col * 3277) >> SIDE
        return src, col - src * QKV_DEV

    def plane_of(src):
        return jnp.where(core == 0, src >> 3, ((src >> 5) << 2) + ((src >> 1) & 3))

    def group_of(src):
        return jnp.where(core == 0, src & 7, (((src >> 3) & 3) << 1) + (src & 1))

    sel_row = iota((WIDE, HEAD), 0)
    for hh in range(10):
        src, part = column_ids(hh)
        sel[:, hh * HEAD:(hh + 1) * HEAD] = jnp.where(sel_row == group_of(src) * ROWS + part, 1.0, 0.0).astype(BF16)

    pos0 = lens_ref[me]
    pos1 = pos0 + 1

    x_val = scatter_plane_end(0)
    x_own[...] = x_val
    gather_plane(0, norm_rows(x_val, gains[0:TILES, :]))

    unf[pl.ds(0, FOLD), :] = ag[0, core, line].astype(F32)
    for s in range(2):
        for t in range(TILES):
            qlhs[s * SIDE:(s + 1) * SIDE, t * LANE:(t + 1) * LANE] = unf[pl.ds(s * TILES + t, SIDE, stride=2 * TILES), :].astype(BF16)
    for k in LINE_ORDER:
        for copy in wf_copies(k, rem(line + LINE - k, LINE), pair_of(k)):
            copy.wait_recv()
    qkv = nt_dot(qlhs[...], wq[...]).astype(BF16).astype(F32)
    qkv = jnp.where((iota((ROWS, WIDE), 1) & 31) < QKV_DEV, qkv, 0.0)
    qmsg[...] = jnp.zeros_like(qmsg)
    for s in range(2):
        for g in range(2):
            qmsg[pl.ds(s * 2 + g, SIDE, stride=SUB), :] = qkv[s * SIDE:(s + 1) * SIDE, g * LANE:(g + 1) * LANE]

    def m_rows(pp):
        return pl.ds(pl.multiple_of(pp * SUB, SUB), SUB)

    def q_copy(k, slot):
        return rcopy(qmsg.at[m_rows(ahead(k))], recv_q.at[m_rows(slot)], q_s.at[k], q_r.at[k], plane_dev(ahead(k)))

    each_plane(lambda k: q_copy(k, plane).start())
    recv_q[m_rows(plane), :] = qmsg[m_rows(plane), :]

    loads[10].wait()
    loads[11].wait()
    step_row = iota((SIDE, LANE), 0) >> 3
    angle = jnp.where(step_row == 0, pos0, pos1).astype(F32) * freq_ref[...]
    cosine = jnp.cos(angle)
    sine = jnp.sin(angle)

    gather_line(0)

    each_plane(lambda k: q_copy(k, behind(k)).wait_recv())
    for s in range(2):
        for g in range(2):
            qrows[s * SIDE:(s + 1) * SIDE, g * LANE:(g + 1) * LANE] = recv_q[pl.ds(s * 2 + g, SIDE, stride=SUB), :].astype(BF16)
    src_row = iota((SIDE, HEAD), 0)
    for hh in range(10):
        wide = nn_dot(qrows[...], sel[:, hh * HEAD:(hh + 1) * HEAD])
        keep = plane_of(column_ids(hh)[0]) == src_row
        for s in range(2):
            vec = jnp.sum(jnp.where(keep, wide[s * SIDE:(s + 1) * SIDE], 0.0), axis=0, keepdims=True)
            at = s * SUB + hh if hh < HEADS else SIDE + (hh - HEADS) * SUB + s
            qkrow[pl.ds(at, 1), :] = vec

    def rotate(vec, cos_val, sin_val):
        first, second = vec[:, :LANE], vec[:, LANE:]
        return jnp.concatenate([first * cos_val - second * sin_val, second * cos_val + first * sin_val], axis=1)

    q_rot = (rotate(qkrow[0:SIDE, :], cosine, sine) * HEAD ** -0.5).astype(BF16)
    cos_k = jnp.concatenate([cosine[0:1], cosine[SUB:9]], axis=0)
    sin_k = jnp.concatenate([sine[0:1], sine[SUB:9]], axis=0)
    k_new = rotate(qkrow[SIDE:18, :], cos_k, sin_k).astype(BF16).astype(F32)
    v_new = qkrow[24:26, :]
    for t in range(SUB):
        rows = slice(t * LANE, (t + 1) * LANE)
        time_id = iota((LANE, HEAD), 0) + t * LANE
        for buf, new in ((kbuf, k_new), (vbuf, v_new)):
            old = buf[rows, :].astype(F32)
            buf[rows, :] = jnp.where(time_id == pos0, new[0:1], jnp.where(time_id == pos1, new[1:2], old)).astype(BF16)
    stores = (pltpu.make_async_copy(kbuf, kout_hbm.at[0], ld.at[12]), pltpu.make_async_copy(vbuf, vout_hbm.at[0], ld.at[13]))
    for copy in stores:
        copy.start()
    scores = nt_dot(q_rot, kbuf[...])
    limit = jnp.where((iota((SIDE, CACHE), 0) >> 3) == 0, pos0, pos1)
    scores = jnp.where(iota((SIDE, CACHE), 1) <= limit, scores, -jnp.inf)
    probs = jnp.exp(scores - jnp.max(scores, axis=1, keepdims=True))
    probs = (probs / jnp.sum(probs, axis=1, keepdims=True)).astype(BF16)
    attn = nn_dot(probs, vbuf[...]).astype(BF16).astype(F32)
    for s in range(2):
        for g in range(2):
            afbuf[pl.ds(s * SIDE + g, SUB, stride=2), :] = attn[s * SUB:(s + 1) * SUB, g * LANE:(g + 1) * LANE]
    for zz in range(LINE):
        for s in range(2):
            amsg[zz, s * LINE:(s + 1) * LINE, :] = afbuf[s * SIDE + zz * LINE:s * SIDE + zz * LINE + LINE, :]

    def a_copy(k, slot):
        return rcopy(amsg.at[div(ahead(k), LINE)], recv_a.at[m_rows(slot)], a_s.at[k], a_r.at[k], plane_dev(ahead(k)))

    each_plane(lambda k: a_copy(k, plane).start())
    recv_a[m_rows(plane), :] = amsg[div(plane, LINE)]

    gather_end(0)
    unfold(0, (other, core))
    up_gate = nt_dot(lhs[...], wgu[...]).astype(BF16).astype(F32)
    gate, up = up_gate[:, :LANE], up_gate[:, LANE:]
    mlp[...] = (jax.nn.silu(gate) * up).astype(BF16)
    for n in range(SUB):
        cols = pl.ds(n * WIDE, WIDE)
        part = nn_dot(mlp[...], wout[pl.ds(ATT_DEV, LANE), cols])
        send_d[1, :, cols] = part[0:LANE].astype(BF16)
        own[:, cols] = part[LANE:WIDE]
    scatter_line(1)

    each_plane(lambda k: a_copy(k, behind(k)).wait_recv())
    for s in range(2):
        for g in range(LINE):
            alhs[s * SIDE:(s + 1) * SIDE, g * LANE:(g + 1) * LANE] = recv_a[pl.ds(s * LINE + g, SIDE, stride=SUB), :].astype(BF16)
    for n in range(SUB):
        cols = pl.ds(n * WIDE, WIDE)
        part = nn_dot(alhs[...], wext[:, :, cols].reshape(FOLD, WIDE))
        for s in range(2):
            for t in range(2):
                afold[pl.ds(s * TILES + n * 2 + t, SIDE, stride=2 * TILES), :] = part[s * SIDE:(s + 1) * SIDE, t * LANE:(t + 1) * LANE]
    scatter_line_end(1)
    fold32[...] += afold[...]
    fold16[1] = fold32[...].astype(BF16)
    scatter_plane(1)

    lane_q = iota((LANE, WIDE), 1)
    sub_b = iota((LANE, WIDE), 0)
    q_core = lane_q >> 7
    q_p = (lane_q >> 1) & 15
    lane_b = (q_p >> 2) * ROWS + (q_p & 3) * (SUB - 6 * q_core) + ((lane_q >> 5) & 3) * (2 + 6 * q_core) + q_core
    lane_s = lane_q & 1
    diag = iota((LANE, LANE), 0) == iota((LANE, LANE), 1)
    next_col = [jnp.sum(jnp.where(diag, next_ref[s:s + 1, :].astype(F32), 0.0), axis=1, keepdims=True) for s in range(2)]
    next_val = jnp.where(lane_s == 0, next_col[0], next_col[1])
    next_lane = jnp.sum(jnp.where(lane_b == sub_b, next_val, 0.0), axis=0, keepdims=True).astype(jnp.int32) - me * VDEV

    out_val = scatter_plane_end(1).astype(BF16).astype(F32)
    gather_plane(1, norm_rows(x_own[...] + out_val, gains[TILES:2 * TILES, :]))
    gather_line(1)
    gather_end(1)
    unfold(1, (0, 1))

    top = jnp.full((1, WIDE), -jnp.inf, F32)
    for n in range(5):
        rows = pl.ds(n * 400, 400)
        part = nt_dot(emb[rows, :], lhs[...]) * D ** -0.5
        lg[rows, :] = part
        top = jnp.maximum(top, jnp.max(part, axis=0, keepdims=True))
    exp_sum = jnp.zeros((1, WIDE), F32)
    target = jnp.zeros((1, WIDE), F32)
    for n in range(5):
        part = lg[pl.ds(n * 400, 400), :]
        exp_sum += jnp.sum(jnp.exp(part - top), axis=0, keepdims=True)
        here = iota((400, WIDE), 0) + n * 400 == next_lane
        target += jnp.sum(jnp.where(here, part, 0.0), axis=0, keepdims=True)
    local_lse = top + jnp.log(exp_sum)

    fin_s[...] = jnp.zeros_like(fin_s)
    for g in range(2):
        fin_s[0, pl.ds(g, 1), :] = local_lse[:, g * LANE:(g + 1) * LANE]
        fin_s[0, pl.ds(2 + g, 1), :] = target[:, g * LANE:(g + 1) * LANE]

    def merge(ref, count):
        high = ref[0]
        for i in range(1, count):
            high = jnp.maximum(high, ref[i])
        scale_sum = jnp.zeros((SUB, LANE), F32)
        plain_sum = jnp.zeros((SUB, LANE), F32)
        for i in range(count):
            scale_sum += jnp.exp(ref[i] - high)
            plain_sum += ref[i]
        return jnp.where(iota((SUB, LANE), 0) < 2, high + jnp.log(scale_sum), plain_sum)

    def fp_copy(k, slot):
        return rcopy(fin_s.at[0], fin_p.at[slot], fp_s.at[k], fp_r.at[k], plane_dev(ahead(k)))

    def ff_copy(k, slot):
        return rcopy(fin_s.at[1], fin_f.at[slot], ff_s.at[k], ff_r.at[k], line_dev(k))

    def fd_copy(slot):
        return rcopy(fin_s.at[2], fin_d.at[slot], fd_s.at[0], fd_r.at[0], partner)

    each_plane(lambda k: fp_copy(k, plane).start())
    fin_p[plane] = fin_s[0]
    each_plane(lambda k: fp_copy(k, behind(k)).wait_recv())
    fin_s[1] = merge(fin_p, SIDE)
    for k in LINE_ORDER:
        ff_copy(k, line).start()
    fin_f[line] = fin_s[1]
    for k in (1, 3, 2):
        ff_copy(k, rem(line + LINE - k, LINE)).wait_recv()
    fin_s[2] = merge(fin_f, LINE)
    fd_copy(core).start()
    fin_d[core] = fin_s[2]
    fd_copy(other).wait_recv()
    final = merge(fin_d, 2)
    lp_row = final[0:1, :]
    lp_lane = jnp.concatenate([final[2:3] - final[0:1], final[3:LINE] - final[1:2]], axis=1)
    for s in range(2):
        col = jnp.sum(jnp.where((lane_b == sub_b) & (lane_s == s), lp_lane, 0.0), axis=1, keepdims=True)
        logp_ref[s:s + 1, :] = jnp.sum(jnp.where(diag, col, 0.0), axis=0, keepdims=True)

    for copy in stores:
        copy.wait()
    for r in range(2):
        for k in range(LINE):
            d_copy(r, k).wait_send()
        for k in range(1, LINE):
            f_copy(r, k).wait_send()
            al_copy(r, k, line).wait_send()
        for k in range(LINE):
            ad_copy(r, k, core, line).wait_send()
        each_plane(lambda k: p_copy(r, k, plane).wait_send())
        each_plane(lambda k: ap_copy(r, k, plane).wait_send())
    for copy in wd_copies():
        copy.wait_send()
    for k in range(1, LINE):
        for copy in wf_copies(k, line, my_pair):
            copy.wait_send()
        ff_copy(k, line).wait_send()
    each_plane(lambda k: q_copy(k, plane).wait_send())
    each_plane(lambda k: a_copy(k, plane).wait_send())
    each_plane(lambda k: fp_copy(k, plane).wait_send())
    fd_copy(core).wait_send()


def solution(mesh):
    def device_fn(tok_ids, next_ids, seq_lens, embed_loc, ln_gain, w_in_loc, w_out_loc, final_gain, k_loc, v_loc):
        half_dim = HEAD // 2
        inv_freq = ROPE_BASE ** (-jnp.arange(half_dim, dtype=F32) / half_dim)
        vmem = pl.BlockSpec(memory_space=pltpu.VMEM)
        smem = pl.BlockSpec(memory_space=pltpu.SMEM)
        hbm = pl.BlockSpec(memory_space=pl.ANY)
        dma = pltpu.SemaphoreType.DMA
        scratch = [
            pltpu.VMEM((VPAD, D), BF16),
            pltpu.VMEM((276, D), BF16),
            pltpu.VMEM((WIDE, D), BF16),
            pltpu.VMEM((144, D), BF16),
            pltpu.VMEM((CACHE, HEAD), BF16),
            pltpu.VMEM((CACHE, HEAD), BF16),
            pltpu.VMEM((WIDE, D), BF16),
            pltpu.VMEM((ROWS, ATT_DEV, D), BF16),
            pltpu.VMEM((WIDE, 2560), BF16),
            pltpu.VMEM((WIDE, VPAD), BF16),
            pltpu.VMEM((2, LANE, D), BF16),
            pltpu.VMEM((LANE, D), F32),
            pltpu.VMEM((2, LINE, ROWS, D), BF16),
            pltpu.VMEM((2, LINE, ROWS, D), BF16),
            pltpu.VMEM((2, LINE, ROWS, D), BF16),
            pltpu.VMEM((ROWS, D), F32),
            pltpu.VMEM((FOLD, LANE), F32),
            pltpu.VMEM((FOLD, LANE), F32),
            pltpu.VMEM((2, FOLD, LANE), BF16),
            pltpu.VMEM((2, SIDE, ROWS, LANE), BF16),
            pltpu.VMEM((ROWS, LANE), F32),
            pltpu.VMEM((ROWS, LANE), F32),
            pltpu.VMEM((2, 2, LINE, FOLD, LANE), BF16),
            pltpu.VMEM((4096, LANE), F32),
            pltpu.VMEM((WIDE, D), BF16),
            pltpu.VMEM((ROWS, D), BF16),
            pltpu.VMEM((LANE, LANE), F32),
            pltpu.VMEM((LANE, LANE), F32),
            pltpu.VMEM((ROWS, WIDE), BF16),
            pltpu.VMEM((ROWS, HEAD), F32),
            pltpu.VMEM((ROWS, LANE), F32),
            pltpu.VMEM((LINE, SUB, LANE), F32),
            pltpu.VMEM((LANE, LANE), F32),
            pltpu.VMEM((ROWS, FOLD), BF16),
            pltpu.VMEM((WIDE, LANE), BF16),
            pltpu.VMEM((VDEV, WIDE), F32),
            pltpu.VMEM((3, SUB, LANE), F32),
            pltpu.VMEM((SIDE, SUB, LANE), F32),
            pltpu.VMEM((LINE, SUB, LANE), F32),
            pltpu.VMEM((2, SUB, LANE), F32),
            dma((14,)),
            dma((2, LINE)), dma((2, LINE)), dma((2, LINE)), dma((2, LINE)), dma((2, SIDE)), dma((2, SIDE)),
            dma((2, SIDE)), dma((2, SIDE)), dma((2, LINE)), dma((2, LINE)), dma((2, LINE)), dma((2, LINE)),
            dma((2,)), dma((2,)), dma((2, LINE)), dma((2, LINE)),
            dma((SIDE,)), dma((SIDE,)), dma((SIDE,)), dma((SIDE,)),
            dma((SIDE,)), dma((SIDE,)), dma((LINE,)), dma((LINE,)), dma((1,)), dma((1,)),
        ]
        return pl.pallas_call(
            kernel,
            out_shape=(jax.ShapeDtypeStruct(tok_ids.shape, F32),
                       jax.ShapeDtypeStruct(k_loc.shape, k_loc.dtype),
                       jax.ShapeDtypeStruct(v_loc.shape, v_loc.dtype)),
            in_specs=[vmem, vmem, smem, hbm, vmem, hbm, hbm, vmem, hbm, hbm, vmem],
            out_specs=(vmem, hbm, hbm),
            scratch_shapes=scratch,
            compiler_params=pltpu.CompilerParams(collective_id=0, has_side_effects=True, vmem_limit_bytes=60 * 2 ** 20),
        )(tok_ids, next_ids, seq_lens, embed_loc, ln_gain.reshape(1, D), w_in_loc.T, w_out_loc, final_gain.reshape(1, D),
          k_loc, v_loc, inv_freq.reshape(1, half_dim))

    cache_spec = P('tp', None, None)
    return jax.shard_map(device_fn, mesh=mesh, in_specs=(P(), P(), P(), P('tp', None), P(), P(None, 'tp'), P('tp', None), P(), cache_spec, cache_spec), out_specs=(P(), cache_spec, cache_spec), check_vma=False)
```

```python
import jax
import jax.numpy as jnp
import numpy as np
from jax import lax
from jax.experimental import pallas as pl
from jax.experimental.pallas import tpu as pltpu
from jax.sharding import PartitionSpec as P

ROPE_BASE = 10000.0
NORM_EPS = 1e-6
F32 = jnp.float32
BF16 = jnp.bfloat16
MESH = pl.DeviceIdType.MESH

D = 2048
VDEV = 2000
VPAD = 2048
HEADS = 8
HEAD = 256
CACHE = 1024
TILES = D // 128
QKV_DEV = 20
ATT_DEV = 16
LANE = 128
WIDE = 256
ROWS = 32
SIDE = 16
LINE = 4
SUB = 8
FOLD = 512
LINE_ORDER = (2, 1, 3)


def rem(value, size):
    return lax.rem(value, jnp.int32(size))


def div(value, size):
    return lax.div(value, jnp.int32(size))


def iota(shape, dim):
    return lax.broadcasted_iota(jnp.int32, shape, dim)


def nt_dot(left, right):
    return lax.dot_general(left, right, (((1,), (1,)), ((), ())), preferred_element_type=F32)


def nn_dot(left, right):
    return lax.dot_general(left, right, (((1,), (0,)), ((), ())), preferred_element_type=F32)


def device_of(core, line, plane):
    return div(plane, LINE) * ROWS + rem(plane, LINE) * (SUB - 6 * core) + line * (2 + 6 * core) + core


def kernel(tok_hbm, next_hbm, lens_hbm, emb_hbm, lng_hbm, win_hbm, wout_hbm, fing_hbm, k_hbm, v_hbm, freq_hbm,
           logp_ref, kbuf, vbuf,
           tok_ref, next_ref, lens_ref, lng_ref, fing_ref, freq_ref,
           emb, win, wgu, wout, wq, wext, sel, hot,
           send_d, own, recv_d, send_f, recv_f, acc, fold32, afold, fold16, recv_p, x_own, gains,
           ag, unf, lhs, qlhs, qmsg, recv_q, qrows, qkrow, afbuf, amsg, recv_a, alhs, mlp, lg,
           fin_s, fin_p, fin_f, fin_d,
           ld, sd_s, sd_r, sf_s, sf_r, sp_s, sp_r, ap_s, ap_r, af_s, af_r, ad_s, ad_r,
           wd_s, wd_r, wf_s, wf_r, q_s, q_r, a_s, a_r, fp_s, fp_r, ff_s, ff_r, fd_s, fd_r):
    me = lax.axis_index('tp')
    core = rem(me, 2)
    other = 1 - core
    zc, yc, xc = div(me, ROWS), rem(div(me, SUB), LINE), rem(div(me, 2), LINE)
    line = xc * other + yc * core
    line_o = yc * other + xc * core
    plane = zc * LINE + yc * other + xc * core
    partner = me + 1 - 2 * core
    me_slot = rem(me, ROWS)
    partner_slot = rem(partner, ROWS)

    def line_dev(k):
        return device_of(core, rem(line + k, LINE), plane)

    def plane_dev(pp):
        return device_of(core, line, pp)

    def rcopy(src, dst, ss, rs, dev):
        return pltpu.make_async_remote_copy(src_ref=src, dst_ref=dst, send_sem=ss, recv_sem=rs, device_id=(dev,), device_id_type=MESH)

    def local_copies():
        small = ((tok_hbm, tok_ref), (next_hbm, next_ref), (lng_hbm, lng_ref), (fing_hbm, fing_ref), (freq_hbm, freq_ref), (lens_hbm, lens_ref))
        out = []
        for n in range(SUB):
            cols = pl.ds(n * WIDE, WIDE)
            out.append(pltpu.make_async_copy(emb_hbm.at[:, cols], emb.at[pl.ds(0, VDEV), cols], ld.at[n]))
        out.append(pltpu.make_async_copy(win_hbm, win, ld.at[SUB]))
        out.append(pltpu.make_async_copy(wout_hbm, wout, ld.at[9]))
        out.append(pltpu.make_async_copy(k_hbm.at[0], kbuf, ld.at[10]))
        out.append(pltpu.make_async_copy(v_hbm.at[0], vbuf, ld.at[11]))
        for n, (src, dst) in enumerate(small):
            out.append(pltpu.make_async_copy(src, dst, ld.at[12 + n]))
        return out

    loads = local_copies()
    for copy in loads[12:] + loads[:12]:
        copy.start()

    wext[...] = jnp.zeros_like(wext)

    barrier = pltpu.get_barrier_semaphore()
    pl.semaphore_signal(barrier, inc=1, device_id=(partner,), device_id_type=MESH)
    for k in range(1, LINE):
        pl.semaphore_signal(barrier, inc=1, device_id=(line_dev(k),), device_id_type=MESH)

    def greet(k, carry):
        pl.semaphore_signal(barrier, inc=1, device_id=(plane_dev(rem(plane + k, SIDE)),), device_id_type=MESH)
        return carry

    lax.fori_loop(1, SIDE, greet, 0)

    for copy in loads[12:]:
        copy.wait()
    emb[pl.ds(VDEV, VPAD - VDEV), :] = jnp.zeros((VPAD - VDEV, D), BF16)
    for t in range(TILES):
        gains[pl.ds(t, 1), :] = lng_ref[t * LANE:(t + 1) * LANE].reshape(1, LANE).astype(F32)
        gains[pl.ds(TILES + t, 1), :] = fing_ref[t * LANE:(t + 1) * LANE].reshape(1, LANE).astype(F32)

    row = iota((WIDE, LANE), 0)
    lane = iota((WIDE, LANE), 1)
    half = row >> 7
    row_core = core + (1 - half) * (1 - 2 * core)
    row_p = (row >> 1) & 15
    row_b = (row_p >> 2) * ROWS + (row_p & 3) * (SUB - 6 * row_core) + ((row >> 5) & 3) * (2 + 6 * row_core) + row_core
    tok_val = jnp.where((row & 1) == 0, tok_ref[0:1, :], tok_ref[1:2, :]).astype(F32)
    tok_col = jnp.sum(jnp.where(lane == row_b, tok_val, 0.0), axis=1, keepdims=True)
    local_col = tok_col.astype(jnp.int32) - me * VDEV
    for t in range(VPAD // LANE):
        hot[:, t * LANE:(t + 1) * LANE] = jnp.where(lane + t * LANE == local_col, 1.0, 0.0).astype(BF16)

    for n in range(LINE):
        cols = pl.ds(n * FOLD, FOLD)
        loads[2 * n].wait()
        loads[2 * n + 1].wait()
        part = nn_dot(hot[...], emb[:, cols])
        send_d[0, :, cols] = part[0:LANE].astype(BF16)
        own[:, cols] = part[LANE:WIDE]

    pl.semaphore_wait(barrier, 19)

    def d_copy(r, k):
        src = pl.ds(pl.multiple_of(rem(line_o + k, LINE) * ROWS, ROWS), ROWS)
        return rcopy(send_d.at[r, src], recv_d.at[r, k], sd_s.at[r, k], sd_r.at[r, k], partner)

    def f_copy(r, k):
        return rcopy(send_f.at[r, k], recv_f.at[r, k], sf_s.at[r, k], sf_r.at[r, k], line_dev(k))

    def scatter_line(r):
        for k in LINE_ORDER + (0,):
            d_copy(r, k).start()
        for k in LINE_ORDER + (0,):
            d_copy(r, k).wait_recv()
            chunk = pl.ds(pl.multiple_of(rem(line + k, LINE) * ROWS, ROWS), ROWS)
            total = own[chunk, :] + recv_d[r, k].astype(F32)
            if k:
                send_f[r, k] = total.astype(BF16)
                f_copy(r, k).start()
            else:
                acc[...] = total

    def scatter_line_end(r):
        for k in (1, 3, 2):
            f_copy(r, k).wait_recv()
            acc[...] += recv_f[r, k].astype(F32)
        for t in range(TILES):
            fold32[pl.ds(t, ROWS, stride=TILES), :] = acc[:, t * LANE:(t + 1) * LANE]

    def each_plane(fn):
        def body(k, carry):
            fn(k)
            return carry
        lax.fori_loop(1, SIDE, body, 0)

    def ahead(k):
        return rem(plane + k, SIDE)

    def behind(k):
        return rem(plane + SIDE - k, SIDE)

    def p_rows(pp):
        return pl.ds(pl.multiple_of(pp * ROWS, ROWS), ROWS)

    def p_copy(r, k, slot):
        return rcopy(fold16.at[r, p_rows(ahead(k))], recv_p.at[r, slot], sp_s.at[r, k], sp_r.at[r, k], plane_dev(ahead(k)))

    def scatter_plane(r):
        each_plane(lambda k: p_copy(r, k, plane).start())

    def scatter_plane_end(r):
        each_plane(lambda k: p_copy(r, k, behind(k)).wait_recv())

        def add(k, total):
            return total + recv_p[r, behind(k)].astype(F32)
        return lax.fori_loop(1, SIDE, add, fold32[p_rows(plane), :])

    def norm_rows(values, gain):
        out = []
        for s in range(2):
            v = values[s * TILES:(s + 1) * TILES]
            v = v - jnp.sum(v, axis=(0, 1), keepdims=True) * (1.0 / D)
            var = jnp.sum(v * v, axis=(0, 1), keepdims=True) * (1.0 / D)
            out.append(v * lax.rsqrt(var + NORM_EPS) * gain)
        return jnp.concatenate(out, axis=0).astype(BF16)

    def ap_copy(r, k, slot):
        ref = ag.at[r, core, line, p_rows(slot)]
        return rcopy(ref, ref, ap_s.at[r, k], ap_r.at[r, k], plane_dev(ahead(k)))

    def al_copy(r, k, slot):
        ref = ag.at[r, core, slot]
        return rcopy(ref, ref, af_s.at[r, k], af_r.at[r, k], line_dev(k))

    def ad_copy(r, k, side, slot):
        ref = ag.at[r, side, slot]
        return rcopy(ref, ref, ad_s.at[r, k], ad_r.at[r, k], partner)

    def gather_plane(r, rows):
        ag[r, core, line, p_rows(plane), :] = rows
        each_plane(lambda k: ap_copy(r, k, plane).start())
        each_plane(lambda k: ap_copy(r, k, behind(k)).wait_recv())
        for k in LINE_ORDER:
            al_copy(r, k, line).start()
        ad_copy(r, 0, core, line).start()

    def gather_line(r):
        for k in (1, 3, 2):
            back = rem(line + LINE - k, LINE)
            al_copy(r, k, back).wait_recv()
            ad_copy(r, k, core, back).start()

    def gather_end(r):
        for k in (0, 1, 3, 2):
            ad_copy(r, k, other, rem(line_o + LINE - k, LINE)).wait_recv()

    def unfold(r, sides):
        for h in range(2):
            for q in range(LINE):
                base = (h * LINE + q) * FOLD
                unf[pl.ds(base, FOLD), :] = ag[r, sides[h], q].astype(F32)
        for t in range(TILES):
            lhs[:, t * LANE:(t + 1) * LANE] = unf[pl.ds(t, WIDE, stride=TILES), :].astype(BF16)

    scatter_line(0)

    loads[SUB].wait()
    loads[9].wait()

    def wq_rows(slot, count):
        return pl.ds(pl.multiple_of(slot * ROWS, ROWS), count * ROWS)

    wq[wq_rows(line * 2 + core, 1), :] = win[0:ROWS, :]
    wext[me_slot] = wout[0:ATT_DEV, :]

    def wd_copies():
        return (rcopy(wq.at[wq_rows(line * 2 + core, 1)], wq.at[wq_rows(line_o * 2 + core, 1)], wd_s.at[0], wd_r.at[0], partner),
                rcopy(wext.at[me_slot], wext.at[me_slot], wd_s.at[1], wd_r.at[1], partner))

    for copy in wd_copies():
        copy.start()

    def wf_copies(k, line_slot, pair_slot):
        q_ref = wq.at[wq_rows(line_slot * 2, 2)]
        e_ref = wext.at[pl.ds(pair_slot, 2)]
        return (rcopy(q_ref, q_ref, wf_s.at[0, k], wf_r.at[0, k], line_dev(k)),
                rcopy(e_ref, e_ref, wf_s.at[1, k], wf_r.at[1, k], line_dev(k)))

    my_pair = me_slot - core

    def pair_of(k):
        return my_pair + (rem(line + LINE - k, LINE) - line) * (2 + 6 * core)

    rcopy(wq.at[wq_rows(line * 2 + core, 1)], wq.at[wq_rows(line * 2 + other, 1)], wd_s.at[0], wd_r.at[0], partner).wait_recv()
    rcopy(wext.at[me_slot], wext.at[partner_slot], wd_s.at[1], wd_r.at[1], partner).wait_recv()
    for k in LINE_ORDER:
        for copy in wf_copies(k, line, my_pair):
            copy.start()

    scatter_line_end(0)
    fold16[0] = fold32[...].astype(BF16)
    scatter_plane(0)

    for t in range(TILES):
        wgu[:, t * LANE:(t + 1) * LANE] = win[QKV_DEV:QKV_DEV + WIDE, t * LANE:(t + 1) * LANE]

    def column_ids(hh):
        col = iota((1, HEAD), 1) + hh * HEAD
        src = (col * 3277) >> SIDE
        return src, col - src * QKV_DEV

    def plane_of(src):
        return jnp.where(core == 0, src >> 3, ((src >> 5) << 2) + ((src >> 1) & 3))

    def group_of(src):
        return jnp.where(core == 0, src & 7, (((src >> 3) & 3) << 1) + (src & 1))

    sel_row = iota((WIDE, HEAD), 0)
    for hh in range(10):
        src, part = column_ids(hh)
        sel[:, hh * HEAD:(hh + 1) * HEAD] = jnp.where(sel_row == group_of(src) * ROWS + part, 1.0, 0.0).astype(BF16)

    pos0 = lens_ref[me]
    pos1 = pos0 + 1

    x_val = scatter_plane_end(0)
    x_own[...] = x_val
    gather_plane(0, norm_rows(x_val, gains[0:TILES, :]))

    unf[pl.ds(0, FOLD), :] = ag[0, core, line].astype(F32)
    for s in range(2):
        for t in range(TILES):
            qlhs[s * SIDE:(s + 1) * SIDE, t * LANE:(t + 1) * LANE] = unf[pl.ds(s * TILES + t, SIDE, stride=2 * TILES), :].astype(BF16)
    for k in LINE_ORDER:
        for copy in wf_copies(k, rem(line + LINE - k, LINE), pair_of(k)):
            copy.wait_recv()
    qkv = nt_dot(qlhs[...], wq[...]).astype(BF16).astype(F32)
    qkv = jnp.where((iota((ROWS, WIDE), 1) & 31) < QKV_DEV, qkv, 0.0)
    qmsg[...] = jnp.zeros_like(qmsg)
    for s in range(2):
        for g in range(2):
            qmsg[pl.ds(s * 2 + g, SIDE, stride=SUB), :] = qkv[s * SIDE:(s + 1) * SIDE, g * LANE:(g + 1) * LANE]

    def m_rows(pp):
        return pl.ds(pl.multiple_of(pp * SUB, SUB), SUB)

    def q_copy(k, slot):
        return rcopy(qmsg.at[m_rows(ahead(k))], recv_q.at[m_rows(slot)], q_s.at[k], q_r.at[k], plane_dev(ahead(k)))

    each_plane(lambda k: q_copy(k, plane).start())
    recv_q[m_rows(plane), :] = qmsg[m_rows(plane), :]

    loads[10].wait()
    loads[11].wait()
    step_row = iota((SIDE, LANE), 0) >> 3
    angle = jnp.where(step_row == 0, pos0, pos1).astype(F32) * freq_ref[...]
    cosine = jnp.cos(angle)
    sine = jnp.sin(angle)

    gather_line(0)

    each_plane(lambda k: q_copy(k, behind(k)).wait_recv())
    for s in range(2):
        for g in range(2):
            qrows[s * SIDE:(s + 1) * SIDE, g * LANE:(g + 1) * LANE] = recv_q[pl.ds(s * 2 + g, SIDE, stride=SUB), :].astype(BF16)
    src_row = iota((SIDE, HEAD), 0)
    for hh in range(10):
        wide = nn_dot(qrows[...], sel[:, hh * HEAD:(hh + 1) * HEAD])
        keep = plane_of(column_ids(hh)[0]) == src_row
        for s in range(2):
            vec = jnp.sum(jnp.where(keep, wide[s * SIDE:(s + 1) * SIDE], 0.0), axis=0, keepdims=True)
            at = s * SUB + hh if hh < HEADS else SIDE + (hh - HEADS) * SUB + s
            qkrow[pl.ds(at, 1), :] = vec

    def rotate(vec, cos_val, sin_val):
        first, second = vec[:, :LANE], vec[:, LANE:]
        return jnp.concatenate([first * cos_val - second * sin_val, second * cos_val + first * sin_val], axis=1)

    q_rot = (rotate(qkrow[0:SIDE, :], cosine, sine) * HEAD ** -0.5).astype(BF16)
    cos_k = jnp.concatenate([cosine[0:1], cosine[SUB:9]], axis=0)
    sin_k = jnp.concatenate([sine[0:1], sine[SUB:9]], axis=0)
    k_new = rotate(qkrow[SIDE:18, :], cos_k, sin_k).astype(BF16).astype(F32)
    v_new = qkrow[24:26, :]
    for t in range(SUB):
        rows = slice(t * LANE, (t + 1) * LANE)
        time_id = iota((LANE, HEAD), 0) + t * LANE
        for buf, new in ((kbuf, k_new), (vbuf, v_new)):
            old = buf[rows, :].astype(F32)
            buf[rows, :] = jnp.where(time_id == pos0, new[0:1], jnp.where(time_id == pos1, new[1:2], old)).astype(BF16)
    scores = nt_dot(q_rot, kbuf[...])
    limit = jnp.where((iota((SIDE, CACHE), 0) >> 3) == 0, pos0, pos1)
    scores = jnp.where(iota((SIDE, CACHE), 1) <= limit, scores, -jnp.inf)
    probs = jnp.exp(scores - jnp.max(scores, axis=1, keepdims=True))
    probs = (probs / jnp.sum(probs, axis=1, keepdims=True)).astype(BF16)
    attn = nn_dot(probs, vbuf[...]).astype(BF16).astype(F32)
    for s in range(2):
        for g in range(2):
            afbuf[pl.ds(s * SIDE + g, SUB, stride=2), :] = attn[s * SUB:(s + 1) * SUB, g * LANE:(g + 1) * LANE]
    for zz in range(LINE):
        for s in range(2):
            amsg[zz, s * LINE:(s + 1) * LINE, :] = afbuf[s * SIDE + zz * LINE:s * SIDE + zz * LINE + LINE, :]

    def a_copy(k, slot):
        return rcopy(amsg.at[div(ahead(k), LINE)], recv_a.at[m_rows(slot)], a_s.at[k], a_r.at[k], plane_dev(ahead(k)))

    each_plane(lambda k: a_copy(k, plane).start())
    recv_a[m_rows(plane), :] = amsg[div(plane, LINE)]

    gather_end(0)
    unfold(0, (other, core))
    up_gate = nt_dot(lhs[...], wgu[...]).astype(BF16).astype(F32)
    gate, up = up_gate[:, :LANE], up_gate[:, LANE:]
    mlp[...] = (jax.nn.silu(gate) * up).astype(BF16)
    for n in range(SUB):
        cols = pl.ds(n * WIDE, WIDE)
        part = nn_dot(mlp[...], wout[pl.ds(ATT_DEV, LANE), cols])
        send_d[1, :, cols] = part[0:LANE].astype(BF16)
        own[:, cols] = part[LANE:WIDE]
    scatter_line(1)

    each_plane(lambda k: a_copy(k, behind(k)).wait_recv())
    for s in range(2):
        for g in range(LINE):
            alhs[s * SIDE:(s + 1) * SIDE, g * LANE:(g + 1) * LANE] = recv_a[pl.ds(s * LINE + g, SIDE, stride=SUB), :].astype(BF16)
    for n in range(SUB):
        cols = pl.ds(n * WIDE, WIDE)
        part = nn_dot(alhs[...], wext[:, :, cols].reshape(FOLD, WIDE))
        for s in range(2):
            for t in range(2):
                afold[pl.ds(s * TILES + n * 2 + t, SIDE, stride=2 * TILES), :] = part[s * SIDE:(s + 1) * SIDE, t * LANE:(t + 1) * LANE]
    scatter_line_end(1)
    fold32[...] += afold[...]
    fold16[1] = fold32[...].astype(BF16)
    scatter_plane(1)

    lane_q = iota((LANE, WIDE), 1)
    sub_b = iota((LANE, WIDE), 0)
    q_core = lane_q >> 7
    q_p = (lane_q >> 1) & 15
    lane_b = (q_p >> 2) * ROWS + (q_p & 3) * (SUB - 6 * q_core) + ((lane_q >> 5) & 3) * (2 + 6 * q_core) + q_core
    lane_s = lane_q & 1
    diag = iota((LANE, LANE), 0) == iota((LANE, LANE), 1)
    next_col = [jnp.sum(jnp.where(diag, next_ref[s:s + 1, :].astype(F32), 0.0), axis=1, keepdims=True) for s in range(2)]
    next_val = jnp.where(lane_s == 0, next_col[0], next_col[1])
    next_lane = jnp.sum(jnp.where(lane_b == sub_b, next_val, 0.0), axis=0, keepdims=True).astype(jnp.int32) - me * VDEV

    out_val = scatter_plane_end(1).astype(BF16).astype(F32)
    gather_plane(1, norm_rows(x_own[...] + out_val, gains[TILES:2 * TILES, :]))
    gather_line(1)
    gather_end(1)
    unfold(1, (0, 1))

    top = jnp.full((1, WIDE), -jnp.inf, F32)
    for n in range(5):
        rows = pl.ds(n * 400, 400)
        part = nt_dot(emb[rows, :], lhs[...]) * D ** -0.5
        lg[rows, :] = part
        top = jnp.maximum(top, jnp.max(part, axis=0, keepdims=True))
    exp_sum = jnp.zeros((1, WIDE), F32)
    target = jnp.zeros((1, WIDE), F32)
    for n in range(5):
        part = lg[pl.ds(n * 400, 400), :]
        exp_sum += jnp.sum(jnp.exp(part - top), axis=0, keepdims=True)
        here = iota((400, WIDE), 0) + n * 400 == next_lane
        target += jnp.sum(jnp.where(here, part, 0.0), axis=0, keepdims=True)
    local_lse = top + jnp.log(exp_sum)

    fin_s[...] = jnp.zeros_like(fin_s)
    for g in range(2):
        fin_s[0, pl.ds(g, 1), :] = local_lse[:, g * LANE:(g + 1) * LANE]
        fin_s[0, pl.ds(2 + g, 1), :] = target[:, g * LANE:(g + 1) * LANE]

    def merge(ref, count):
        high = ref[0]
        for i in range(1, count):
            high = jnp.maximum(high, ref[i])
        scale_sum = jnp.zeros((SUB, LANE), F32)
        plain_sum = jnp.zeros((SUB, LANE), F32)
        for i in range(count):
            scale_sum += jnp.exp(ref[i] - high)
            plain_sum += ref[i]
        return jnp.where(iota((SUB, LANE), 0) < 2, high + jnp.log(scale_sum), plain_sum)

    def fp_copy(k, slot):
        return rcopy(fin_s.at[0], fin_p.at[slot], fp_s.at[k], fp_r.at[k], plane_dev(ahead(k)))

    def ff_copy(k, slot):
        return rcopy(fin_s.at[1], fin_f.at[slot], ff_s.at[k], ff_r.at[k], line_dev(k))

    def fd_copy(slot):
        return rcopy(fin_s.at[2], fin_d.at[slot], fd_s.at[0], fd_r.at[0], partner)

    each_plane(lambda k: fp_copy(k, plane).start())
    fin_p[plane] = fin_s[0]
    each_plane(lambda k: fp_copy(k, behind(k)).wait_recv())
    fin_s[1] = merge(fin_p, SIDE)
    for k in LINE_ORDER:
        ff_copy(k, line).start()
    fin_f[line] = fin_s[1]
    for k in (1, 3, 2):
        ff_copy(k, rem(line + LINE - k, LINE)).wait_recv()
    fin_s[2] = merge(fin_f, LINE)
    fd_copy(core).start()
    fin_d[core] = fin_s[2]
    fd_copy(other).wait_recv()
    final = merge(fin_d, 2)
    lp_row = final[0:1, :]
    lp_lane = jnp.concatenate([final[2:3] - final[0:1], final[3:LINE] - final[1:2]], axis=1)
    for s in range(2):
        col = jnp.sum(jnp.where((lane_b == sub_b) & (lane_s == s), lp_lane, 0.0), axis=1, keepdims=True)
        logp_ref[s:s + 1, :] = jnp.sum(jnp.where(diag, col, 0.0), axis=0, keepdims=True)

    for r in range(2):
        for k in range(LINE):
            d_copy(r, k).wait_send()
        for k in range(1, LINE):
            f_copy(r, k).wait_send()
            al_copy(r, k, line).wait_send()
        for k in range(LINE):
            ad_copy(r, k, core, line).wait_send()
        each_plane(lambda k: p_copy(r, k, plane).wait_send())
        each_plane(lambda k: ap_copy(r, k, plane).wait_send())
    for copy in wd_copies():
        copy.wait_send()
    for k in range(1, LINE):
        for copy in wf_copies(k, line, my_pair):
            copy.wait_send()
        ff_copy(k, line).wait_send()
    each_plane(lambda k: q_copy(k, plane).wait_send())
    each_plane(lambda k: a_copy(k, plane).wait_send())
    each_plane(lambda k: fp_copy(k, plane).wait_send())
    fd_copy(core).wait_send()


def finish(logp_ref, kbuf, vbuf, logp_out, kout_hbm, vout_hbm, sems):
    copies = [pltpu.make_async_copy(kbuf, kout_hbm.at[0], sems.at[0]), pltpu.make_async_copy(vbuf, vout_hbm.at[0], sems.at[1])]
    for copy in copies:
        copy.start()
    logp_out[...] = logp_ref[...]
    for copy in copies:
        copy.wait()


def solution(mesh):
    def device_fn(tok_ids, next_ids, seq_lens, embed_loc, ln_gain, w_in_loc, w_out_loc, final_gain, k_loc, v_loc):
        half_dim = HEAD // 2
        inv_freq = np.power(np.float32(ROPE_BASE), -np.arange(half_dim, dtype=np.float32) / half_dim).reshape(1, half_dim)
        vmem = pl.BlockSpec(memory_space=pltpu.VMEM)
        hbm = pl.BlockSpec(memory_space=pltpu.HBM)
        dma = pltpu.SemaphoreType.DMA
        scratch = [
            pltpu.VMEM(tok_ids.shape, jnp.int32),
            pltpu.VMEM(next_ids.shape, jnp.int32),
            pltpu.SMEM(seq_lens.shape, jnp.int32),
            pltpu.VMEM((D,), BF16),
            pltpu.VMEM((D,), BF16),
            pltpu.VMEM((1, half_dim), F32),
            pltpu.VMEM((VPAD, D), BF16),
            pltpu.VMEM((276, D), BF16),
            pltpu.VMEM((WIDE, D), BF16),
            pltpu.VMEM((144, D), BF16),
            pltpu.VMEM((WIDE, D), BF16),
            pltpu.VMEM((ROWS, ATT_DEV, D), BF16),
            pltpu.VMEM((WIDE, 2560), BF16),
            pltpu.VMEM((WIDE, VPAD), BF16),
            pltpu.VMEM((2, LANE, D), BF16),
            pltpu.VMEM((LANE, D), F32),
            pltpu.VMEM((2, LINE, ROWS, D), BF16),
            pltpu.VMEM((2, LINE, ROWS, D), BF16),
            pltpu.VMEM((2, LINE, ROWS, D), BF16),
            pltpu.VMEM((ROWS, D), F32),
            pltpu.VMEM((FOLD, LANE), F32),
            pltpu.VMEM((FOLD, LANE), F32),
            pltpu.VMEM((2, FOLD, LANE), BF16),
            pltpu.VMEM((2, SIDE, ROWS, LANE), BF16),
            pltpu.VMEM((ROWS, LANE), F32),
            pltpu.VMEM((ROWS, LANE), F32),
            pltpu.VMEM((2, 2, LINE, FOLD, LANE), BF16),
            pltpu.VMEM((4096, LANE), F32),
            pltpu.VMEM((WIDE, D), BF16),
            pltpu.VMEM((ROWS, D), BF16),
            pltpu.VMEM((LANE, LANE), F32),
            pltpu.VMEM((LANE, LANE), F32),
            pltpu.VMEM((ROWS, WIDE), BF16),
            pltpu.VMEM((ROWS, HEAD), F32),
            pltpu.VMEM((ROWS, LANE), F32),
            pltpu.VMEM((LINE, SUB, LANE), F32),
            pltpu.VMEM((LANE, LANE), F32),
            pltpu.VMEM((ROWS, FOLD), BF16),
            pltpu.VMEM((WIDE, LANE), BF16),
            pltpu.VMEM((VDEV, WIDE), F32),
            pltpu.VMEM((3, SUB, LANE), F32),
            pltpu.VMEM((SIDE, SUB, LANE), F32),
            pltpu.VMEM((LINE, SUB, LANE), F32),
            pltpu.VMEM((2, SUB, LANE), F32),
            dma((18,)),
            dma((2, LINE)), dma((2, LINE)), dma((2, LINE)), dma((2, LINE)), dma((2, SIDE)), dma((2, SIDE)),
            dma((2, SIDE)), dma((2, SIDE)), dma((2, LINE)), dma((2, LINE)), dma((2, LINE)), dma((2, LINE)),
            dma((2,)), dma((2,)), dma((2, LINE)), dma((2, LINE)),
            dma((SIDE,)), dma((SIDE,)), dma((SIDE,)), dma((SIDE,)),
            dma((SIDE,)), dma((SIDE,)), dma((LINE,)), dma((LINE,)), dma((1,)), dma((1,)),
        ]
        logp, k_done, v_done = pl.pallas_call(
            kernel,
            out_shape=(jax.ShapeDtypeStruct(tok_ids.shape, F32),
                       jax.ShapeDtypeStruct(k_loc.shape[1:], k_loc.dtype),
                       jax.ShapeDtypeStruct(v_loc.shape[1:], v_loc.dtype)),
            in_specs=[hbm] * 11,
            out_specs=(vmem, vmem, vmem),
            scratch_shapes=scratch,
            compiler_params=pltpu.CompilerParams(collective_id=0, has_side_effects=True, vmem_limit_bytes=48 * 2 ** 20),
        )(*[pltpu.with_memory_space_constraint(arr, pltpu.HBM) for arr in (tok_ids, next_ids, seq_lens, embed_loc, ln_gain, w_in_loc.T, w_out_loc, final_gain,
          k_loc, v_loc, inv_freq)])
        return pl.pallas_call(
            finish,
            out_shape=(jax.ShapeDtypeStruct(tok_ids.shape, F32),
                       jax.ShapeDtypeStruct(k_loc.shape, k_loc.dtype),
                       jax.ShapeDtypeStruct(v_loc.shape, v_loc.dtype)),
            in_specs=[vmem, vmem, vmem],
            out_specs=(vmem, pl.BlockSpec(memory_space=pl.ANY), pl.BlockSpec(memory_space=pl.ANY)),
            scratch_shapes=[dma((2,))],
            compiler_params=pltpu.CompilerParams(vmem_limit_bytes=8 * 2 ** 20),
        )(logp, k_done, v_done)

    cache_spec = P('tp', None, None)
    return jax.shard_map(device_fn, mesh=mesh, in_specs=(P(), P(), P(), P('tp', None), P(), P(None, 'tp'), P('tp', None), P(), cache_spec, cache_spec), out_specs=(P(), cache_spec, cache_spec), check_vma=False)
```

```python
import jax
import jax.numpy as jnp
import numpy as np
from jax import lax
from jax.experimental import pallas as pl
from jax.experimental.pallas import tpu as pltpu
from jax.sharding import PartitionSpec as P

ROPE_BASE = 10000.0
NORM_EPS = 1e-6
F32 = jnp.float32
BF16 = jnp.bfloat16
MESH = pl.DeviceIdType.MESH

D = 2048
VDEV = 2000
VPAD = 2048
HEADS = 8
HEAD = 256
CACHE = 1024
TILES = D // 128
QKV_DEV = 20
ATT_DEV = 16
LANE = 128
WIDE = 256
ROWS = 32
SIDE = 16
LINE = 4
SUB = 8
FOLD = 512
LINE_ORDER = (2, 1, 3)
ARRIVE = (1, 3, 2)
FAR = (2, 1, 3, 0)
NEAR = (0, 1, 3, 2)


def rem(value, size):
    return lax.rem(value, jnp.int32(size))


def div(value, size):
    return lax.div(value, jnp.int32(size))


def iota(shape, dim):
    return lax.broadcasted_iota(jnp.int32, shape, dim)


def nt_dot(left, right):
    return lax.dot_general(left, right, (((1,), (1,)), ((), ())), preferred_element_type=F32)


def nn_dot(left, right):
    return lax.dot_general(left, right, (((1,), (0,)), ((), ())), preferred_element_type=F32)


def device_of(core, line, plane):
    return div(plane, LINE) * ROWS + rem(plane, LINE) * (SUB - 6 * core) + line * (2 + 6 * core) + core


def kernel(tok_hbm, next_hbm, lens_hbm, emb_hbm, lng_hbm, win_hbm, wout_hbm, fing_hbm, k_hbm, v_hbm, freq_hbm,
           logp_ref, kbuf, vbuf,
           tok_ref, next_ref, lens_ref, lng_ref, fing_ref, freq_ref,
           emb, win, wgu, wout, wq, wext, sel, hot,
           send_d, own, recv_d, send_f, recv_f, total, fold32, afold, fold16, recv_p, x_own, gains,
           ag, unf, lhs, qlhs, qmsg, recv_q, qrows, qkrow, afbuf, amsg, recv_a, alhs, mlp, lg,
           fin_s, fin_p, fin_f, fin_d,
           ld, sd_s, sd_r, sf_s, sf_r, sp_s, sp_r, ap_s, ap_r, af_s, af_r, ad_s, ad_r,
           wd_s, wd_r, wf_s, wf_r, q_s, q_r, a_s, a_r, fp_s, fp_r, ff_s, ff_r, fd_s, fd_r):
    me = lax.axis_index('tp')
    core = rem(me, 2)
    other = 1 - core
    zc, yc, xc = div(me, ROWS), rem(div(me, SUB), LINE), rem(div(me, 2), LINE)
    line = xc * other + yc * core
    line_o = yc * other + xc * core
    wc = yc * other + xc * core
    plane = zc * LINE + wc
    partner = me + 1 - 2 * core
    me_slot = rem(me, ROWS)
    partner_slot = rem(partner, ROWS)

    def fwd(place, k):
        return rem(place + k, LINE)

    def bck(place, k):
        return rem(place + LINE - k, LINE)

    def block(index, size):
        return pl.ds(pl.multiple_of(index * size, size), size)

    def zw_dev(zz, ww):
        return zz * ROWS + ww * (SUB - 6 * core) + line * (2 + 6 * core) + core

    def line_dev(k):
        return device_of(core, rem(line + k, LINE), plane)

    def plane_dev(pp):
        return device_of(core, line, pp)

    def rcopy(src, dst, ss, rs, dev):
        return pltpu.make_async_remote_copy(src_ref=src, dst_ref=dst, send_sem=ss, recv_sem=rs, device_id=(dev,), device_id_type=MESH)

    def local_copies():
        small = ((tok_hbm, tok_ref), (next_hbm, next_ref), (lng_hbm, lng_ref), (fing_hbm, fing_ref), (freq_hbm, freq_ref), (lens_hbm, lens_ref))
        out = []
        for n in range(SUB):
            cols = pl.ds(n * WIDE, WIDE)
            out.append(pltpu.make_async_copy(emb_hbm.at[:, cols], emb.at[pl.ds(0, VDEV), cols], ld.at[n]))
        out.append(pltpu.make_async_copy(win_hbm, win, ld.at[SUB]))
        out.append(pltpu.make_async_copy(wout_hbm, wout, ld.at[9]))
        out.append(pltpu.make_async_copy(k_hbm.at[0], kbuf, ld.at[10]))
        out.append(pltpu.make_async_copy(v_hbm.at[0], vbuf, ld.at[11]))
        for n, (src, dst) in enumerate(small):
            out.append(pltpu.make_async_copy(src, dst, ld.at[12 + n]))
        return out

    loads = local_copies()
    for copy in loads[12:] + loads[:12]:
        copy.start()

    wext[...] = jnp.zeros_like(wext)

    barrier = pltpu.get_barrier_semaphore()
    pl.semaphore_signal(barrier, inc=1, device_id=(partner,), device_id_type=MESH)
    for k in range(1, LINE):
        pl.semaphore_signal(barrier, inc=1, device_id=(line_dev(k),), device_id_type=MESH)

    def greet(k, carry):
        pl.semaphore_signal(barrier, inc=1, device_id=(plane_dev(rem(plane + k, SIDE)),), device_id_type=MESH)
        return carry

    lax.fori_loop(1, SIDE, greet, 0)

    for copy in loads[12:]:
        copy.wait()
    emb[pl.ds(VDEV, VPAD - VDEV), :] = jnp.zeros((VPAD - VDEV, D), BF16)
    for t in range(TILES):
        gains[pl.ds(t, 1), :] = lng_ref[t * LANE:(t + 1) * LANE].reshape(1, LANE).astype(F32)
        gains[pl.ds(TILES + t, 1), :] = fing_ref[t * LANE:(t + 1) * LANE].reshape(1, LANE).astype(F32)

    def sequence_of(index, own_core):
        return ((index >> 5) & 3) * ROWS + ((index >> 1) & 3) * (SUB - 6 * own_core) + ((index >> 3) & 3) * (2 + 6 * own_core) + own_core

    def half_core(index):
        return core + (1 - (index >> 7)) * (1 - 2 * core)

    row = iota((WIDE, LANE), 0)
    lane = iota((WIDE, LANE), 1)
    row_b = sequence_of(row, half_core(row))
    tok_val = jnp.where((row & 1) == 0, tok_ref[0:1, :], tok_ref[1:2, :]).astype(F32)
    tok_col = jnp.sum(jnp.where(lane == row_b, tok_val, 0.0), axis=1, keepdims=True)
    local_col = tok_col.astype(jnp.int32) - me * VDEV
    for t in range(VPAD // LANE):
        hot[:, t * LANE:(t + 1) * LANE] = jnp.where(lane + t * LANE == local_col, 1.0, 0.0).astype(BF16)

    def d_cols(n):
        cols = pl.ds(n * FOLD, FOLD)
        return rcopy(send_d.at[0, :, cols], recv_d.at[0, :, cols], sd_s.at[0, n], sd_r.at[0, n], partner)

    for n in range(LINE):
        cols = pl.ds(n * FOLD, FOLD)
        loads[2 * n].wait()
        loads[2 * n + 1].wait()
        part = nn_dot(hot[...], emb[:, cols])
        send_d[0, :, cols] = part[0:LANE].astype(BF16)
        own[:, cols] = part[LANE:WIDE]
        if n == 2:
            pl.semaphore_wait(barrier, 19)
            for m in range(n):
                d_cols(m).start()
        if n >= 2:
            d_cols(n).start()

    def d_rows(d):
        rows = block(fwd(zc, d), ROWS)
        return rcopy(send_d.at[1, rows], recv_d.at[1, rows], sd_s.at[1, d], sd_r.at[1, d], partner)

    def f_copy(r, k, d):
        return rcopy(send_f.at[r, k, d], recv_f.at[r, k, d], sf_s.at[r, k, d], sf_r.at[r, k, d], line_dev(k))

    def p_copy(r, d, e):
        at = d * LINE + e
        return rcopy(fold16.at[r, d, block(fwd(wc, e), ROWS)], recv_p.at[r, at], sp_s.at[r, at], sp_r.at[r, at], zw_dev(fwd(zc, d), fwd(wc, e)))

    def scatter_send(r):
        for d in FAR:
            rows = block(fwd(zc, d), ROWS)
            if r:
                d_rows(d).wait_recv()
            total[d] = own[rows, :] + recv_d[r, rows, :].astype(F32)
            for k in LINE_ORDER:
                send_f[r, k, d] = total[d, block(fwd(line, k), SUB), :].astype(BF16)
                f_copy(r, k, d).start()

    def scatter_turn(r):
        for d in FAR:
            part = total[d, block(line, SUB), :]
            for k in ARRIVE:
                f_copy(r, k, d).wait_recv()
                part = part + recv_f[r, k, d].astype(F32)
            for t in range(TILES):
                fold32[d, pl.ds(t, SUB, stride=TILES), :] = part[:, t * LANE:(t + 1) * LANE]
            if r:
                fold32[d] += afold[block(fwd(zc, d), LANE), :]
            fold16[r, d] = fold32[d].astype(BF16)
            for e in FAR:
                if d or e:
                    p_copy(r, d, e).start()

    def scatter_end(r):
        out = fold32[0, block(wc, ROWS), :]
        for d in NEAR:
            for e in NEAR:
                if d or e:
                    p_copy(r, d, e).wait_recv()
                    out = out + recv_p[r, d * LINE + e].astype(F32)
        return out

    def each_plane(fn):
        def body(k, carry):
            fn(k)
            return carry
        lax.fori_loop(1, SIDE, body, 0)

    def ahead(k):
        return rem(plane + k, SIDE)

    def behind(k):
        return rem(plane + SIDE - k, SIDE)

    def norm_rows(values, gain):
        out = []
        for s in range(2):
            v = values[s * TILES:(s + 1) * TILES]
            v = v - jnp.sum(v, axis=(0, 1), keepdims=True) * (1.0 / D)
            var = jnp.sum(v * v, axis=(0, 1), keepdims=True) * (1.0 / D)
            out.append(v * lax.rsqrt(var + NORM_EPS) * gain)
        return jnp.concatenate(out, axis=0).astype(BF16)

    def ap_copy(r, d, e, zz, rows):
        ref = ag.at[r, core, line, zz, rows]
        return rcopy(ref, ref, ap_s.at[r, d * LINE + e], ap_r.at[r, d if d else LINE + e], zw_dev(fwd(zc, d), fwd(wc, e)))

    def al_copy(r, k, d, place, zz):
        ref = ag.at[r, core, place, zz]
        return rcopy(ref, ref, af_s.at[r, k, d], af_r.at[r, k, d], line_dev(k))

    def ad_copy(r, k, d, side, place, zz):
        ref = ag.at[r, side, place, zz]
        return rcopy(ref, ref, ad_s.at[r, k, d], ad_r.at[r, k, d], partner)

    def gather_plane(r, rows):
        ag[r, core, line, zc, block(wc, ROWS), :] = rows
        for d in FAR:
            for e in FAR:
                if d or e:
                    ap_copy(r, d, e, zc, block(wc, ROWS)).start()
        for d in NEAR:
            zz = bck(zc, d)
            if d:
                ap_copy(r, d, 0, zz, pl.ds(0, LANE)).wait_recv()
            else:
                for e in ARRIVE:
                    ap_copy(r, 0, e, zc, block(bck(wc, e), ROWS)).wait_recv()
            for k in LINE_ORDER:
                al_copy(r, k, d, line, zz).start()
            ad_copy(r, 0, d, core, line, zz).start()

    def gather_line(r):
        for d in NEAR:
            zz = bck(zc, d)
            for k in ARRIVE:
                al_copy(r, k, d, bck(line, k), zz).wait_recv()
                ad_copy(r, k, d, core, bck(line, k), zz).start()

    def gather_end(r):
        for d in NEAR:
            for k in (0,) + ARRIVE:
                ad_copy(r, k, d, other, bck(line_o, k), bck(zc, d)).wait_recv()

    def unfold(r, h, side):
        for zz in range(LINE):
            for f in range(LINE):
                unf[pl.ds(((h * LINE + zz) * LINE + f) * LANE, LANE), :] = ag[r, side, f, zz].astype(F32)
        for t in range(TILES):
            lhs[h * LANE:(h + 1) * LANE, t * LANE:(t + 1) * LANE] = unf[pl.ds(h * D + t, LANE, stride=TILES), :].astype(BF16)

    for n in range(LINE):
        d_cols(n).wait_recv()
    scatter_send(0)

    loads[SUB].wait()
    loads[9].wait()

    def wq_rows(slot, count):
        return pl.ds(pl.multiple_of(slot * ROWS, ROWS), count * ROWS)

    wq[wq_rows(line * 2 + core, 1), :] = win[0:ROWS, :]
    wext[me_slot] = wout[0:ATT_DEV, :]

    def wd_copies():
        return (rcopy(wq.at[wq_rows(line * 2 + core, 1)], wq.at[wq_rows(line_o * 2 + core, 1)], wd_s.at[0], wd_r.at[0], partner),
                rcopy(wext.at[me_slot], wext.at[me_slot], wd_s.at[1], wd_r.at[1], partner))

    for copy in wd_copies():
        copy.start()

    def wf_copies(k, line_slot, pair_slot):
        q_ref = wq.at[wq_rows(line_slot * 2, 2)]
        e_ref = wext.at[pl.ds(pair_slot, 2)]
        return (rcopy(q_ref, q_ref, wf_s.at[0, k], wf_r.at[0, k], line_dev(k)),
                rcopy(e_ref, e_ref, wf_s.at[1, k], wf_r.at[1, k], line_dev(k)))

    my_pair = me_slot - core

    def pair_of(k):
        return my_pair + (rem(line + LINE - k, LINE) - line) * (2 + 6 * core)

    rcopy(wq.at[wq_rows(line * 2 + core, 1)], wq.at[wq_rows(line * 2 + other, 1)], wd_s.at[0], wd_r.at[0], partner).wait_recv()
    rcopy(wext.at[me_slot], wext.at[partner_slot], wd_s.at[1], wd_r.at[1], partner).wait_recv()
    for k in LINE_ORDER:
        for copy in wf_copies(k, line, my_pair):
            copy.start()

    scatter_turn(0)

    for t in range(TILES):
        wgu[:, t * LANE:(t + 1) * LANE] = win[QKV_DEV:QKV_DEV + WIDE, t * LANE:(t + 1) * LANE]

    def column_ids(hh):
        col = iota((1, HEAD), 1) + hh * HEAD
        src = (col * 3277) >> SIDE
        return src, col - src * QKV_DEV

    def plane_of(src):
        return jnp.where(core == 0, src >> 3, ((src >> 5) << 2) + ((src >> 1) & 3))

    def group_of(src):
        return jnp.where(core == 0, src & 7, (((src >> 3) & 3) << 1) + (src & 1))

    sel_row = iota((WIDE, HEAD), 0)
    for hh in range(10):
        src, part = column_ids(hh)
        sel[:, hh * HEAD:(hh + 1) * HEAD] = jnp.where(sel_row == group_of(src) * ROWS + part, 1.0, 0.0).astype(BF16)

    pos0 = lens_ref[me]
    pos1 = pos0 + 1

    x_val = scatter_end(0)
    x_own[...] = x_val
    gather_plane(0, norm_rows(x_val, gains[0:TILES, :]))

    for zz in range(LINE):
        unf[pl.ds(zz * LANE, LANE), :] = ag[0, core, line, zz].astype(F32)
    for s in range(2):
        for t in range(TILES):
            qlhs[s * SIDE:(s + 1) * SIDE, t * LANE:(t + 1) * LANE] = unf[pl.ds(s * TILES + t, SIDE, stride=2 * TILES), :].astype(BF16)
    for k in LINE_ORDER:
        for copy in wf_copies(k, rem(line + LINE - k, LINE), pair_of(k)):
            copy.wait_recv()
    qkv = nt_dot(qlhs[...], wq[...]).astype(BF16).astype(F32)
    qkv = jnp.where((iota((ROWS, WIDE), 1) & 31) < QKV_DEV, qkv, 0.0)
    qmsg[...] = jnp.zeros_like(qmsg)
    for s in range(2):
        for g in range(2):
            qmsg[pl.ds(s * 2 + g, SIDE, stride=SUB), :] = qkv[s * SIDE:(s + 1) * SIDE, g * LANE:(g + 1) * LANE]

    def m_rows(pp):
        return pl.ds(pl.multiple_of(pp * SUB, SUB), SUB)

    def q_copy(k, slot):
        return rcopy(qmsg.at[m_rows(ahead(k))], recv_q.at[m_rows(slot)], q_s.at[k], q_r.at[k], plane_dev(ahead(k)))

    each_plane(lambda k: q_copy(k, plane).start())
    recv_q[m_rows(plane), :] = qmsg[m_rows(plane), :]

    loads[10].wait()
    loads[11].wait()
    step_row = iota((SIDE, LANE), 0) >> 3
    angle = jnp.where(step_row == 0, pos0, pos1).astype(F32) * freq_ref[...]
    cosine = jnp.cos(angle)
    sine = jnp.sin(angle)

    gather_line(0)
    unfold(0, 1, core)
    gather_end(0)
    unfold(0, 0, other)
    up_gate = nt_dot(lhs[...], wgu[...]).astype(BF16).astype(F32)
    gate, up = up_gate[:, :LANE], up_gate[:, LANE:]
    mlp[...] = (jax.nn.silu(gate) * up).astype(BF16)
    for d in FAR:
        rows = block(fwd(zc, d), ROWS)
        rows_own = pl.ds(pl.multiple_of(LANE + fwd(zc, d) * ROWS, ROWS), ROWS)
        part = nn_dot(jnp.concatenate([mlp[rows, :], mlp[rows_own, :]], axis=0), wout[ATT_DEV:ATT_DEV + LANE, :])
        send_d[1, rows, :] = part[0:ROWS].astype(BF16)
        own[rows, :] = part[ROWS:2 * ROWS]
        d_rows(d).start()

    each_plane(lambda k: q_copy(k, behind(k)).wait_recv())
    for s in range(2):
        for g in range(2):
            qrows[s * SIDE:(s + 1) * SIDE, g * LANE:(g + 1) * LANE] = recv_q[pl.ds(s * 2 + g, SIDE, stride=SUB), :].astype(BF16)
    src_row = iota((SIDE, HEAD), 0)
    for hh in range(10):
        wide = nn_dot(qrows[...], sel[:, hh * HEAD:(hh + 1) * HEAD])
        keep = plane_of(column_ids(hh)[0]) == src_row
        for s in range(2):
            vec = jnp.sum(jnp.where(keep, wide[s * SIDE:(s + 1) * SIDE], 0.0), axis=0, keepdims=True)
            at = s * SUB + hh if hh < HEADS else SIDE + (hh - HEADS) * SUB + s
            qkrow[pl.ds(at, 1), :] = vec

    def rotate(vec, cos_val, sin_val):
        first, second = vec[:, :LANE], vec[:, LANE:]
        return jnp.concatenate([first * cos_val - second * sin_val, second * cos_val + first * sin_val], axis=1)

    q_rot = (rotate(qkrow[0:SIDE, :], cosine, sine) * HEAD ** -0.5).astype(BF16)
    cos_k = jnp.concatenate([cosine[0:1], cosine[SUB:9]], axis=0)
    sin_k = jnp.concatenate([sine[0:1], sine[SUB:9]], axis=0)
    k_new = rotate(qkrow[SIDE:18, :], cos_k, sin_k).astype(BF16).astype(F32)
    v_new = qkrow[24:26, :]
    for t in range(SUB):
        rows = slice(t * LANE, (t + 1) * LANE)
        time_id = iota((LANE, HEAD), 0) + t * LANE
        for buf, new in ((kbuf, k_new), (vbuf, v_new)):
            old = buf[rows, :].astype(F32)
            buf[rows, :] = jnp.where(time_id == pos0, new[0:1], jnp.where(time_id == pos1, new[1:2], old)).astype(BF16)
    scores = nt_dot(q_rot, kbuf[...])
    limit = jnp.where((iota((SIDE, CACHE), 0) >> 3) == 0, pos0, pos1)
    scores = jnp.where(iota((SIDE, CACHE), 1) <= limit, scores, -jnp.inf)
    probs = jnp.exp(scores - jnp.max(scores, axis=1, keepdims=True))
    probs = (probs / jnp.sum(probs, axis=1, keepdims=True)).astype(BF16)
    attn = nn_dot(probs, vbuf[...]).astype(BF16).astype(F32)
    for s in range(2):
        for g in range(2):
            afbuf[pl.ds(s * SIDE + g, SUB, stride=2), :] = attn[s * SUB:(s + 1) * SUB, g * LANE:(g + 1) * LANE]
    for zz in range(LINE):
        for s in range(2):
            amsg[zz, s * LINE:(s + 1) * LINE, :] = afbuf[s * SIDE + zz * LINE:s * SIDE + zz * LINE + LINE, :]

    def a_copy(k, slot):
        return rcopy(amsg.at[div(ahead(k), LINE)], recv_a.at[m_rows(slot)], a_s.at[k], a_r.at[k], plane_dev(ahead(k)))

    each_plane(lambda k: a_copy(k, plane).start())
    recv_a[m_rows(plane), :] = amsg[div(plane, LINE)]

    scatter_send(1)

    each_plane(lambda k: a_copy(k, behind(k)).wait_recv())
    for s in range(2):
        for g in range(LINE):
            alhs[s * SIDE:(s + 1) * SIDE, g * LANE:(g + 1) * LANE] = recv_a[pl.ds(s * LINE + g, SIDE, stride=SUB), :].astype(BF16)
    for n in range(SUB):
        cols = pl.ds(n * WIDE, WIDE)
        part = nn_dot(alhs[...], wext[:, :, cols].reshape(FOLD, WIDE))
        for s in range(2):
            for t in range(2):
                afold[pl.ds(s * TILES + n * 2 + t, SIDE, stride=2 * TILES), :] = part[s * SIDE:(s + 1) * SIDE, t * LANE:(t + 1) * LANE]
    scatter_turn(1)

    lane_q = iota((LANE, WIDE), 1)
    sub_b = iota((LANE, WIDE), 0)
    lane_b = sequence_of(lane_q, half_core(lane_q))
    lane_s = lane_q & 1
    diag = iota((LANE, LANE), 0) == iota((LANE, LANE), 1)
    next_col = [jnp.sum(jnp.where(diag, next_ref[s:s + 1, :].astype(F32), 0.0), axis=1, keepdims=True) for s in range(2)]
    next_val = jnp.where(lane_s == 0, next_col[0], next_col[1])
    next_lane = jnp.sum(jnp.where(lane_b == sub_b, next_val, 0.0), axis=0, keepdims=True).astype(jnp.int32) - me * VDEV

    out_val = scatter_end(1).astype(BF16).astype(F32)
    gather_plane(1, norm_rows(x_own[...] + out_val, gains[TILES:2 * TILES, :]))
    gather_line(1)
    unfold(1, 1, core)
    gather_end(1)
    unfold(1, 0, other)

    top = jnp.full((1, WIDE), -jnp.inf, F32)
    for n in range(5):
        rows = pl.ds(n * 400, 400)
        part = nt_dot(emb[rows, :], lhs[...]) * D ** -0.5
        lg[rows, :] = part
        top = jnp.maximum(top, jnp.max(part, axis=0, keepdims=True))
    exp_sum = jnp.zeros((1, WIDE), F32)
    target = jnp.zeros((1, WIDE), F32)
    for n in range(5):
        part = lg[pl.ds(n * 400, 400), :]
        exp_sum += jnp.sum(jnp.exp(part - top), axis=0, keepdims=True)
        here = iota((400, WIDE), 0) + n * 400 == next_lane
        target += jnp.sum(jnp.where(here, part, 0.0), axis=0, keepdims=True)
    local_lse = top + jnp.log(exp_sum)

    fin_s[...] = jnp.zeros_like(fin_s)
    for g in range(2):
        for at, vec in ((g, local_lse), (2 + g, target)):
            fin_s[0, pl.ds(at, 1), :] = jnp.where(core == g, vec[:, LANE:], vec[:, :LANE])

    def merge(ref, count):
        high = ref[0]
        for i in range(1, count):
            high = jnp.maximum(high, ref[i])
        scale_sum = jnp.zeros((SUB, LANE), F32)
        plain_sum = jnp.zeros((SUB, LANE), F32)
        for i in range(count):
            scale_sum += jnp.exp(ref[i] - high)
            plain_sum += ref[i]
        return jnp.where(iota((SUB, LANE), 0) < 2, high + jnp.log(scale_sum), plain_sum)

    def fp_copy(k, slot):
        return rcopy(fin_s.at[0], fin_p.at[slot], fp_s.at[k], fp_r.at[k], plane_dev(ahead(k)))

    def ff_copy(k, slot):
        return rcopy(fin_s.at[1], fin_f.at[slot], ff_s.at[k], ff_r.at[k], line_dev(k))

    def fd_copy(slot):
        return rcopy(fin_s.at[2], fin_d.at[slot], fd_s.at[0], fd_r.at[0], partner)

    each_plane(lambda k: fp_copy(k, plane).start())
    fin_p[plane] = fin_s[0]
    each_plane(lambda k: fp_copy(k, behind(k)).wait_recv())
    fin_s[1] = merge(fin_p, SIDE)
    for k in LINE_ORDER:
        ff_copy(k, line).start()
    fin_f[line] = fin_s[1]
    for k in (1, 3, 2):
        ff_copy(k, rem(line + LINE - k, LINE)).wait_recv()
    fin_s[2] = merge(fin_f, LINE)
    fd_copy(core).start()
    fin_d[core] = fin_s[2]
    fd_copy(other).wait_recv()
    final = merge(fin_d, 2)
    lane_b = sequence_of(lane_q, lane_q >> 7)
    lp_lane = jnp.concatenate([final[2:3] - final[0:1], final[3:LINE] - final[1:2]], axis=1)
    for s in range(2):
        col = jnp.sum(jnp.where((lane_b == sub_b) & (lane_s == s), lp_lane, 0.0), axis=1, keepdims=True)
        logp_ref[s:s + 1, :] = jnp.sum(jnp.where(diag, col, 0.0), axis=0, keepdims=True)

    for n in range(LINE):
        d_cols(n).wait_send()
        d_rows(n).wait_send()
    for r in range(2):
        for d in range(LINE):
            for k in range(LINE):
                if k:
                    f_copy(r, k, d).wait_send()
                    al_copy(r, k, d, line, bck(zc, d)).wait_send()
                ad_copy(r, k, d, core, line, bck(zc, d)).wait_send()
                if d or k:
                    p_copy(r, d, k).wait_send()
                    ap_copy(r, d, k, zc, block(wc, ROWS)).wait_send()
    for copy in wd_copies():
        copy.wait_send()
    for k in range(1, LINE):
        for copy in wf_copies(k, line, my_pair):
            copy.wait_send()
        ff_copy(k, line).wait_send()
    each_plane(lambda k: q_copy(k, plane).wait_send())
    each_plane(lambda k: a_copy(k, plane).wait_send())
    each_plane(lambda k: fp_copy(k, plane).wait_send())
    fd_copy(core).wait_send()


def finish(logp_ref, kbuf, vbuf, logp_out, kout_hbm, vout_hbm, sems):
    copies = [pltpu.make_async_copy(kbuf, kout_hbm.at[0], sems.at[0]), pltpu.make_async_copy(vbuf, vout_hbm.at[0], sems.at[1])]
    for copy in copies:
        copy.start()
    logp_out[...] = logp_ref[...]
    for copy in copies:
        copy.wait()


def solution(mesh):
    def device_fn(tok_ids, next_ids, seq_lens, embed_loc, ln_gain, w_in_loc, w_out_loc, final_gain, k_loc, v_loc):
        half_dim = HEAD // 2
        inv_freq = np.power(np.float32(ROPE_BASE), -np.arange(half_dim, dtype=np.float32) / half_dim).reshape(1, half_dim)
        vmem = pl.BlockSpec(memory_space=pltpu.VMEM)
        hbm = pl.BlockSpec(memory_space=pltpu.HBM)
        dma = pltpu.SemaphoreType.DMA
        scratch = [
            pltpu.VMEM(tok_ids.shape, jnp.int32),
            pltpu.VMEM(next_ids.shape, jnp.int32),
            pltpu.SMEM(seq_lens.shape, jnp.int32),
            pltpu.VMEM((D,), BF16),
            pltpu.VMEM((D,), BF16),
            pltpu.VMEM((1, half_dim), F32),
            pltpu.VMEM((VPAD, D), BF16),
            pltpu.VMEM((276, D), BF16),
            pltpu.VMEM((WIDE, D), BF16),
            pltpu.VMEM((144, D), BF16),
            pltpu.VMEM((WIDE, D), BF16),
            pltpu.VMEM((ROWS, ATT_DEV, D), BF16),
            pltpu.VMEM((WIDE, 2560), BF16),
            pltpu.VMEM((WIDE, VPAD), BF16),
            pltpu.VMEM((2, LANE, D), BF16),
            pltpu.VMEM((LANE, D), F32),
            pltpu.VMEM((2, LANE, D), BF16),
            pltpu.VMEM((2, LINE, LINE, SUB, D), BF16),
            pltpu.VMEM((2, LINE, LINE, SUB, D), BF16),
            pltpu.VMEM((LINE, ROWS, D), F32),
            pltpu.VMEM((LINE, LANE, LANE), F32),
            pltpu.VMEM((FOLD, LANE), F32),
            pltpu.VMEM((2, LINE, LANE, LANE), BF16),
            pltpu.VMEM((2, SIDE, ROWS, LANE), BF16),
            pltpu.VMEM((ROWS, LANE), F32),
            pltpu.VMEM((ROWS, LANE), F32),
            pltpu.VMEM((2, 2, LINE, LINE, LANE, LANE), BF16),
            pltpu.VMEM((4096, LANE), F32),
            pltpu.VMEM((WIDE, D), BF16),
            pltpu.VMEM((ROWS, D), BF16),
            pltpu.VMEM((LANE, LANE), F32),
            pltpu.VMEM((LANE, LANE), F32),
            pltpu.VMEM((ROWS, WIDE), BF16),
            pltpu.VMEM((ROWS, HEAD), F32),
            pltpu.VMEM((ROWS, LANE), F32),
            pltpu.VMEM((LINE, SUB, LANE), F32),
            pltpu.VMEM((LANE, LANE), F32),
            pltpu.VMEM((ROWS, FOLD), BF16),
            pltpu.VMEM((WIDE, LANE), BF16),
            pltpu.VMEM((VDEV, WIDE), F32),
            pltpu.VMEM((3, SUB, LANE), F32),
            pltpu.VMEM((SIDE, SUB, LANE), F32),
            pltpu.VMEM((LINE, SUB, LANE), F32),
            pltpu.VMEM((2, SUB, LANE), F32),
            dma((18,)),
            dma((2, LINE)), dma((2, LINE)), *[dma((2, LINE, LINE)) for _ in range(2)], dma((2, SIDE)), dma((2, SIDE)),
            dma((2, SIDE)), dma((2, SUB)), *[dma((2, LINE, LINE)) for _ in range(LINE)],
            dma((2,)), dma((2,)), dma((2, LINE)), dma((2, LINE)),
            dma((SIDE,)), dma((SIDE,)), dma((SIDE,)), dma((SIDE,)),
            dma((SIDE,)), dma((SIDE,)), dma((LINE,)), dma((LINE,)), dma((1,)), dma((1,)),
        ]
        logp, k_done, v_done = pl.pallas_call(
            kernel,
            out_shape=(jax.ShapeDtypeStruct(tok_ids.shape, F32),
                       jax.ShapeDtypeStruct(k_loc.shape[1:], k_loc.dtype),
                       jax.ShapeDtypeStruct(v_loc.shape[1:], v_loc.dtype)),
            in_specs=[hbm] * 11,
            out_specs=(vmem, vmem, vmem),
            scratch_shapes=scratch,
            compiler_params=pltpu.CompilerParams(collective_id=0, has_side_effects=True, vmem_limit_bytes=48 * 2 ** 20),
        )(*[pltpu.with_memory_space_constraint(arr, pltpu.HBM) for arr in (tok_ids, next_ids, seq_lens, embed_loc, ln_gain, w_in_loc.T, w_out_loc, final_gain,
          k_loc, v_loc, inv_freq)])
        return pl.pallas_call(
            finish,
            out_shape=(jax.ShapeDtypeStruct(tok_ids.shape, F32),
                       jax.ShapeDtypeStruct(k_loc.shape, k_loc.dtype),
                       jax.ShapeDtypeStruct(v_loc.shape, v_loc.dtype)),
            in_specs=[vmem, vmem, vmem],
            out_specs=(vmem, pl.BlockSpec(memory_space=pl.ANY), pl.BlockSpec(memory_space=pl.ANY)),
            scratch_shapes=[dma((2,))],
            compiler_params=pltpu.CompilerParams(vmem_limit_bytes=8 * 2 ** 20),
        )(logp, k_done, v_done)

    cache_spec = P('tp', None, None)
    return jax.shard_map(device_fn, mesh=mesh, in_specs=(P(), P(), P(), P('tp', None), P(), P(None, 'tp'), P('tp', None), P(), cache_spec, cache_spec), out_specs=(P(), cache_spec, cache_spec), check_vma=False)
```

```python
import functools

import jax
import jax.numpy as jnp
import numpy as np
from jax import lax
from jax.experimental import pallas as pl
from jax.experimental.pallas import tpu as pltpu
from jax.sharding import PartitionSpec as P

ROPE_BASE = 10000.0
NORM_EPS = 1e-6
F32 = jnp.float32
BF16 = jnp.bfloat16
MESH = pl.DeviceIdType.MESH

D = 2048
VDEV = 2000
VPAD = 2048
HEADS = 8
HEAD = 256
CACHE = 1024
TILES = D // 128
QKV_DEV = 20
ATT_DEV = 16
LANE = 128
WIDE = 256
ROWS = 32
SIDE = 16
LINE = 4
SUB = 8
FOLD = 512
STEPS = 2
LINE_ORDER = (2, 1, 3)
ARRIVE = (1, 3, 2)
FAR = (2, 1, 3, 0)
NEAR = (0, 1, 3, 2)
OTHERS = pl.ds(1, 3)
THREE = pl.ds(0, 3)
FIFTEEN = pl.ds(0, 15)
FARTHER = pl.ds(LINE, 12)
PEERS = pl.ds(0, 120)


def rem(value, size):
    return lax.rem(value, jnp.int32(size))


def div(value, size):
    return lax.div(value, jnp.int32(size))


def iota(shape, dim):
    return lax.broadcasted_iota(jnp.int32, shape, dim)


def nt_dot(left, right):
    return lax.dot_general(left, right, (((1,), (1,)), ((), ())), preferred_element_type=F32)


def nn_dot(left, right):
    return lax.dot_general(left, right, (((1,), (0,)), ((), ())), preferred_element_type=F32)


def device_of(core, line, plane):
    return div(plane, LINE) * ROWS + rem(plane, LINE) * (SUB - 6 * core) + line * (2 + 6 * core) + core


def kernel(tok_hbm, next_hbm, lens_hbm, emb_hbm, lng_hbm, win_hbm, wout_hbm, fing_hbm, k_hbm, v_hbm, freq_hbm,
           logp_ref, kbuf, vbuf,
           tok_ref, next_ref, lens_ref, lng_ref, fing_ref, freq_ref,
           emb, win, wgu, wout, wq, wext, sel, hot,
           send_d, own, recv_d, send_f, recv_f, total, fold32, afold, fold16, recv_p, x_own, gains,
           ag, unf, lhs, qlhs, qmsg, recv_q, qrows, qkrow, afbuf, amsg, recv_a, alhs, mlp,
           fin_s, fin_p, fin_f, fin_d,
           ld, sd_s, sd_r, sf_s, sf_r, sp_s, sp_r, ap_s, ap_r, af_s, af_r, ad_s, ad_r,
           wd_s, wd_r, wf_s, wf_r, q_s, q_r, a_s, a_r, fp_s, fp_r, ff_s, ff_r, fd_s, fd_r):
    me = lax.axis_index('tp')
    core = rem(me, 2)
    other = 1 - core
    zc, yc, xc = div(me, ROWS), rem(div(me, SUB), LINE), rem(div(me, 2), LINE)
    line = xc * other + yc * core
    line_o = yc * other + xc * core
    wc = yc * other + xc * core
    plane = zc * LINE + wc
    partner = me + 1 - 2 * core
    me_slot = rem(me, ROWS)
    partner_slot = rem(partner, ROWS)

    def fwd(place, k):
        return rem(place + k, LINE)

    def bck(place, k):
        return rem(place + LINE - k, LINE)

    def block(index, size):
        return pl.ds(pl.multiple_of(index * size, size), size)

    def zw_dev(zz, ww):
        return zz * ROWS + ww * (SUB - 6 * core) + line * (2 + 6 * core) + core

    def line_dev(k):
        return device_of(core, rem(line + k, LINE), plane)

    def plane_dev(pp):
        return device_of(core, line, pp)

    def rcopy(src, dst, ss, rs, dev):
        return pltpu.make_async_remote_copy(src_ref=src, dst_ref=dst, send_sem=ss, recv_sem=rs, device_id=(dev,), device_id_type=MESH)

    def take(ref, sem):
        pltpu.make_async_copy(ref, ref, sem).wait()

    def local_copies():
        small = ((tok_hbm, tok_ref), (next_hbm, next_ref), (lng_hbm, lng_ref), (fing_hbm, fing_ref), (freq_hbm, freq_ref), (lens_hbm, lens_ref))
        out = []
        for n in range(LINE):
            cols = pl.ds(n * FOLD, FOLD)
            out.append(pltpu.make_async_copy(emb_hbm.at[:, cols], emb.at[pl.ds(0, VDEV), cols], ld.at[n]))
        out.append(pltpu.make_async_copy(win_hbm, win, ld.at[4]))
        out.append(pltpu.make_async_copy(wout_hbm, wout, ld.at[5]))
        out.append(pltpu.make_async_copy(k_hbm.at[0], kbuf, ld.at[6]))
        out.append(pltpu.make_async_copy(v_hbm.at[0], vbuf, ld.at[7]))
        for n, (src, dst) in enumerate(small):
            out.append(pltpu.make_async_copy(src, dst, ld.at[8 + n]))
        return out

    loads = local_copies()
    for copy in loads[8:] + loads[:8]:
        copy.start()

    wext[...] = jnp.zeros_like(wext)
    wq[...] = jnp.zeros_like(wq)

    barrier = pltpu.get_barrier_semaphore()
    pl.semaphore_signal(barrier, inc=1, device_id=(partner,), device_id_type=MESH)
    for k in range(1, LINE):
        pl.semaphore_signal(barrier, inc=1, device_id=(line_dev(k),), device_id_type=MESH)

    def greet(k, carry):
        pl.semaphore_signal(barrier, inc=1, device_id=(plane_dev(rem(plane + k, SIDE)),), device_id_type=MESH)
        return carry

    lax.fori_loop(1, SIDE, greet, 0)

    for copy in loads[8:]:
        copy.wait()
    emb[pl.ds(VDEV, VPAD - VDEV), :] = jnp.zeros((VPAD - VDEV, D), BF16)
    for t in range(TILES):
        gains[pl.ds(t, 1), :] = lng_ref[t * LANE:(t + 1) * LANE].reshape(1, LANE).astype(F32)
        gains[pl.ds(TILES + t, 1), :] = fing_ref[t * LANE:(t + 1) * LANE].reshape(1, LANE).astype(F32)

    def sequence_of(index, own_core):
        return ((index >> 5) & 3) * ROWS + ((index >> 1) & 3) * (SUB - 6 * own_core) + ((index >> 3) & 3) * (2 + 6 * own_core) + own_core

    def half_core(index):
        return core + (1 - (index >> 7)) * (1 - 2 * core)

    row = iota((WIDE, LANE), 0)
    lane = iota((WIDE, LANE), 1)
    row_b = sequence_of(row, half_core(row))
    tok_val = jnp.where((row & 1) == 0, tok_ref[0:1, :], tok_ref[1:2, :]).astype(F32)
    tok_col = jnp.sum(jnp.where(lane == row_b, tok_val, 0.0), axis=1, keepdims=True)
    local_col = tok_col.astype(jnp.int32) - me * VDEV
    for t in range(VPAD // LANE):
        hot[:, t * LANE:(t + 1) * LANE] = jnp.where(lane + t * LANE == local_col, 1.0, 0.0).astype(BF16)

    def d_cols(n):
        cols = pl.ds(n * FOLD, FOLD)
        return rcopy(send_d.at[0, :, cols], recv_d.at[0, :, cols], sd_s.at[0], sd_r.at[0], partner)

    for n in range(LINE):
        cols = pl.ds(n * FOLD, FOLD)
        loads[n].wait()
        part = nn_dot(hot[...], emb[:, cols])
        send_d[0, :, cols] = part[0:LANE].astype(BF16)
        own[:, cols] = part[LANE:WIDE]
        if n == 2:
            pl.semaphore_wait(barrier, 19)
            for m in range(n):
                d_cols(m).start()
        if n >= 2:
            d_cols(n).start()

    def d_rows(d):
        rows = block(fwd(zc, d), ROWS)
        return rcopy(send_d.at[1, rows], recv_d.at[1, rows], sd_s.at[1], sd_r.at[1 + d], partner)

    def f_copy(r, k, d):
        return rcopy(send_f.at[r, k, d], recv_f.at[r, k, d], sf_s.at[r], sf_r.at[r, d], line_dev(k))

    def p_copy(r, d, e):
        at = d * LINE + e
        return rcopy(fold16.at[r, d, block(fwd(wc, e), ROWS)], recv_p.at[r, at], sp_s.at[r, min(d, 1)], sp_r.at[r, min(d, 1)], zw_dev(fwd(zc, d), fwd(wc, e)))

    def scatter_send(r):
        for d in FAR:
            rows = block(fwd(zc, d), ROWS)
            if r:
                d_rows(d).wait_recv()
            total[d] = own[rows, :] + recv_d[r, rows, :].astype(F32)
            for k in LINE_ORDER:
                send_f[r, k, d] = total[d, block(fwd(line, k), SUB), :].astype(BF16)
                f_copy(r, k, d).start()

    def scatter_turn(r):
        for d in FAR:
            part = total[d, block(line, SUB), :]
            take(recv_f.at[r, OTHERS, d], sf_r.at[r, d])
            for k in ARRIVE:
                part = part + recv_f[r, k, d].astype(F32)
            for t in range(TILES):
                fold32[d, pl.ds(t, SUB, stride=TILES), :] = part[:, t * LANE:(t + 1) * LANE]
            if r:
                fold32[d] += afold[block(fwd(zc, d), LANE), :]
            fold16[r, d] = fold32[d].astype(BF16)
            for e in FAR:
                if d or e:
                    p_copy(r, d, e).start()

    def scatter_end(r):
        out = fold32[0, block(wc, ROWS), :]
        take(recv_p.at[r, OTHERS], sp_r.at[r, 0])
        take(recv_p.at[r, FARTHER], sp_r.at[r, 1])
        for at in range(1, SIDE):
            out = out + recv_p[r, at].astype(F32)
        return out

    def each_plane(fn):
        def body(k, carry):
            fn(k)
            return carry
        lax.fori_loop(1, SIDE, body, 0)

    def ahead(k):
        return rem(plane + k, SIDE)

    def behind(k):
        return rem(plane + SIDE - k, SIDE)

    def norm_rows(values, gain):
        out = []
        for s in range(STEPS):
            v = values[s * TILES:(s + 1) * TILES]
            v = v - jnp.sum(v, axis=(0, 1), keepdims=True) * (1.0 / D)
            var = jnp.sum(v * v, axis=(0, 1), keepdims=True) * (1.0 / D)
            out.append(v * lax.rsqrt(var + NORM_EPS) * gain)
        return jnp.concatenate(out, axis=0).astype(BF16)

    def ap_copy(r, d, e, zz, rows):
        ref = ag.at[r, core, line, zz, rows]
        return rcopy(ref, ref, ap_s.at[r, min(d, 1)], ap_r.at[r, d], zw_dev(fwd(zc, d), fwd(wc, e)))

    def al_copy(r, k, d, place, zz):
        ref = ag.at[r, core, place, zz]
        return rcopy(ref, ref, af_s.at[r], af_r.at[r, d], line_dev(k))

    def ad_copy(r, side, place, zz):
        ref = ag.at[r, side, place, zz]
        return rcopy(ref, ref, ad_s.at[r], ad_r.at[r], partner)

    def gather_plane(r, rows):
        ag[r, core, line, zc, block(wc, ROWS), :] = rows
        for d in FAR:
            for e in FAR:
                if d or e:
                    ap_copy(r, d, e, zc, block(wc, ROWS)).start()
        for d in NEAR:
            zz = bck(zc, d)
            take(ag.at[r, core, line, zz, pl.ds(0, LANE if d else 3 * ROWS)], ap_r.at[r, d])
            for k in LINE_ORDER:
                al_copy(r, k, d, line, zz).start()
            ad_copy(r, core, line, zz).start()

    def gather_line(r):
        for d in NEAR:
            zz = bck(zc, d)
            take(ag.at[r, core, THREE, zz], af_r.at[r, d])
            for k in ARRIVE:
                ad_copy(r, core, bck(line, k), zz).start()

    def gather_end(r):
        take(ag.at[r, other], ad_r.at[r])

    def unfold(r, h, side):
        for zz in range(LINE):
            for f in range(LINE):
                unf[pl.ds(((h * LINE + zz) * LINE + f) * LANE, LANE), :] = ag[r, side, f, zz].astype(F32)
        for t in range(TILES):
            lhs[h * LANE:(h + 1) * LANE, t * LANE:(t + 1) * LANE] = unf[pl.ds(h * D + t, LANE, stride=TILES), :].astype(BF16)

    take(recv_d.at[0], sd_r.at[0])
    scatter_send(0)

    loads[4].wait()
    loads[5].wait()

    def wq_rows(slot, count):
        return pl.ds(pl.multiple_of(slot * ROWS, ROWS), count * ROWS)

    wq[wq_rows(line * 2 + core, 1), :] = win[0:ROWS, :]
    wext[me_slot] = wout[0:ATT_DEV, :]
    my_pair = me_slot - core

    def wd_copies():
        return (rcopy(wq.at[wq_rows(line * 2 + core, 1)], wq.at[wq_rows(line_o * 2 + core, 1)], wd_s.at[0], wd_r.at[0], partner),
                rcopy(wext.at[me_slot], wext.at[me_slot], wd_s.at[0], wd_r.at[0], partner))

    def wq_copy(k, g):
        ref = wq.at[pl.ds(pl.multiple_of((line * 2 + g) * ROWS, ROWS), 24)]
        return rcopy(ref, ref, wf_s.at[0], wf_r.at[0], line_dev(k))

    def wext_copy(k):
        ref = wext.at[pl.ds(my_pair, 2)]
        return rcopy(ref, ref, wf_s.at[1], wf_r.at[1], line_dev(k))

    for copy in wd_copies():
        copy.start()
    take(wext.at[THREE], wd_r.at[0])
    for k in LINE_ORDER:
        for g in range(STEPS):
            wq_copy(k, g).start()

    scatter_turn(0)

    for t in range(TILES):
        wgu[:, t * LANE:(t + 1) * LANE] = win[QKV_DEV:QKV_DEV + WIDE, t * LANE:(t + 1) * LANE]

    def column_ids(hh):
        col = iota((1, HEAD), 1) + hh * HEAD
        src = (col * 3277) >> SIDE
        return src, col - src * QKV_DEV

    def plane_of(src):
        return jnp.where(core == 0, src >> 3, ((src >> 5) << 2) + ((src >> 1) & 3))

    def group_of(src):
        return jnp.where(core == 0, src & 7, (((src >> 3) & 3) << 1) + (src & 1))

    sel_row = iota((WIDE, HEAD), 0)
    for hh in range(10):
        src, part = column_ids(hh)
        sel[:, hh * HEAD:(hh + 1) * HEAD] = jnp.where(sel_row == group_of(src) * ROWS + part, 1.0, 0.0).astype(BF16)

    pos0 = lens_ref[me]
    pos1 = pos0 + 1

    x_val = scatter_end(0)
    x_own[...] = x_val
    gather_plane(0, norm_rows(x_val, gains[0:TILES, :]))

    for zz in range(LINE):
        unf[pl.ds(zz * LANE, LANE), :] = ag[0, core, line, zz].astype(F32)
    for s in range(STEPS):
        for t in range(TILES):
            qlhs[s * SIDE:(s + 1) * SIDE, t * LANE:(t + 1) * LANE] = unf[pl.ds(s * TILES + t, SIDE, stride=2 * TILES), :].astype(BF16)
    take(wext.at[pl.ds(0, 9)], wf_r.at[0])
    qkv = nt_dot(qlhs[...], wq[...]).astype(BF16).astype(F32)
    qkv = jnp.where((iota((ROWS, WIDE), 1) & 31) < QKV_DEV, qkv, 0.0)
    qmsg[...] = jnp.zeros_like(qmsg)
    for s in range(STEPS):
        for g in range(STEPS):
            qmsg[pl.ds(s * 2 + g, SIDE, stride=SUB), :] = qkv[s * SIDE:(s + 1) * SIDE, g * LANE:(g + 1) * LANE]

    def m_rows(pp):
        return pl.ds(pl.multiple_of(pp * SUB, SUB), SUB)

    def q_copy(k, slot):
        return rcopy(qmsg.at[m_rows(ahead(k))], recv_q.at[m_rows(slot)], q_s.at[0], q_r.at[0], plane_dev(ahead(k)))

    each_plane(lambda k: q_copy(k, plane).start())
    recv_q[m_rows(plane), :] = qmsg[m_rows(plane), :]

    loads[6].wait()
    loads[7].wait()
    step_row = iota((SIDE, LANE), 0) >> 3
    angle = jnp.where(step_row == 0, pos0, pos1).astype(F32) * freq_ref[...]
    cosine = jnp.cos(angle)
    sine = jnp.sin(angle)

    gather_line(0)
    for k in LINE_ORDER:
        wext_copy(k).start()

    take(recv_q.at[PEERS], q_r.at[0])
    for s in range(STEPS):
        for g in range(STEPS):
            qrows[s * SIDE:(s + 1) * SIDE, g * LANE:(g + 1) * LANE] = recv_q[pl.ds(s * 2 + g, SIDE, stride=SUB), :].astype(BF16)
    src_row = iota((SIDE, HEAD), 0)
    for hh in range(10):
        wide = nn_dot(qrows[...], sel[:, hh * HEAD:(hh + 1) * HEAD])
        keep = plane_of(column_ids(hh)[0]) == src_row
        for s in range(STEPS):
            vec = jnp.sum(jnp.where(keep, wide[s * SIDE:(s + 1) * SIDE], 0.0), axis=0, keepdims=True)
            at = s * SUB + hh if hh < HEADS else SIDE + (hh - HEADS) * SUB + s
            qkrow[pl.ds(at, 1), :] = vec

    def rotate(vec, cos_val, sin_val):
        first, second = vec[:, :LANE], vec[:, LANE:]
        return jnp.concatenate([first * cos_val - second * sin_val, second * cos_val + first * sin_val], axis=1)

    q_rot = (rotate(qkrow[0:SIDE, :], cosine, sine) * HEAD ** -0.5).astype(BF16)
    cos_k = jnp.concatenate([cosine[0:1], cosine[SUB:9]], axis=0)
    sin_k = jnp.concatenate([sine[0:1], sine[SUB:9]], axis=0)
    k_new = rotate(qkrow[SIDE:18, :], cos_k, sin_k).astype(BF16).astype(F32)
    v_new = qkrow[24:26, :]
    for t in range(SUB):
        rows = slice(t * LANE, (t + 1) * LANE)
        time_id = iota((LANE, HEAD), 0) + t * LANE
        for buf, new in ((kbuf, k_new), (vbuf, v_new)):
            old = buf[rows, :].astype(F32)
            buf[rows, :] = jnp.where(time_id == pos0, new[0:1], jnp.where(time_id == pos1, new[1:2], old)).astype(BF16)
    scores = nt_dot(q_rot, kbuf[...])
    limit = jnp.where((iota((SIDE, CACHE), 0) >> 3) == 0, pos0, pos1)
    scores = jnp.where(iota((SIDE, CACHE), 1) <= limit, scores, -jnp.inf)
    probs = jnp.exp(scores - jnp.max(scores, axis=1, keepdims=True))
    probs = (probs / jnp.sum(probs, axis=1, keepdims=True)).astype(BF16)
    attn = nn_dot(probs, vbuf[...]).astype(BF16).astype(F32)
    for s in range(STEPS):
        for g in range(STEPS):
            afbuf[pl.ds(s * SIDE + g, SUB, stride=2), :] = attn[s * SUB:(s + 1) * SUB, g * LANE:(g + 1) * LANE]
    for zz in range(LINE):
        for s in range(STEPS):
            amsg[zz, s * LINE:(s + 1) * LINE, :] = afbuf[s * SIDE + zz * LINE:s * SIDE + zz * LINE + LINE, :]

    def a_copy(k, slot):
        return rcopy(amsg.at[div(ahead(k), LINE)], recv_a.at[m_rows(slot)], a_s.at[0], a_r.at[0], plane_dev(ahead(k)))

    each_plane(lambda k: a_copy(k, plane).start())
    recv_a[m_rows(plane), :] = amsg[div(plane, LINE)]

    unfold(0, 1, core)
    gather_end(0)
    unfold(0, 0, other)
    up_gate = nt_dot(lhs[...], wgu[...]).astype(BF16).astype(F32)
    gate, up = up_gate[:, :LANE], up_gate[:, LANE:]
    mlp[...] = (jax.nn.silu(gate) * up).astype(BF16)
    for d in FAR:
        rows = block(fwd(zc, d), ROWS)
        rows_own = pl.ds(pl.multiple_of(LANE + fwd(zc, d) * ROWS, ROWS), ROWS)
        part = nn_dot(jnp.concatenate([mlp[rows, :], mlp[rows_own, :]], axis=0), wout[ATT_DEV:ATT_DEV + LANE, :])
        send_d[1, rows, :] = part[0:ROWS].astype(BF16)
        own[rows, :] = part[ROWS:2 * ROWS]
        d_rows(d).start()

    scatter_send(1)

    take(wext.at[pl.ds(0, 6)], wf_r.at[1])
    take(recv_a.at[PEERS], a_r.at[0])
    for s in range(STEPS):
        for g in range(LINE):
            alhs[s * SIDE:(s + 1) * SIDE, g * LANE:(g + 1) * LANE] = recv_a[pl.ds(s * LINE + g, SIDE, stride=SUB), :].astype(BF16)
    for n in range(SUB):
        cols = pl.ds(n * WIDE, WIDE)
        part = nn_dot(alhs[...], wext[:, :, cols].reshape(FOLD, WIDE))
        for s in range(STEPS):
            for t in range(STEPS):
                afold[pl.ds(s * TILES + n * 2 + t, SIDE, stride=2 * TILES), :] = part[s * SIDE:(s + 1) * SIDE, t * LANE:(t + 1) * LANE]
    scatter_turn(1)

    lane_q = iota((LANE, WIDE), 1)
    sub_b = iota((LANE, WIDE), 0)
    lane_b = sequence_of(lane_q, half_core(lane_q))
    lane_s = lane_q & 1
    diag = iota((LANE, LANE), 0) == iota((LANE, LANE), 1)
    next_col = [jnp.sum(jnp.where(diag, next_ref[s:s + 1, :].astype(F32), 0.0), axis=1, keepdims=True) for s in range(STEPS)]
    next_val = jnp.where(lane_s == 0, next_col[0], next_col[1])
    next_lane = jnp.sum(jnp.where(lane_b == sub_b, next_val, 0.0), axis=0, keepdims=True).astype(jnp.int32) - me * VDEV

    out_val = scatter_end(1).astype(BF16).astype(F32)
    gather_plane(1, norm_rows(x_own[...] + out_val, gains[TILES:2 * TILES, :]))
    gather_line(1)
    unfold(1, 1, core)
    gather_end(1)
    unfold(1, 0, other)

    tops, sums = [], []
    target = jnp.zeros((1, WIDE), F32)
    for n in range(5):
        part = nt_dot(emb[pl.ds(n * 400, 400), :], lhs[...]) * D ** -0.5
        tops.append(jnp.max(part, axis=0, keepdims=True))
        sums.append(jnp.sum(jnp.exp(part - tops[n]), axis=0, keepdims=True))
        here = iota((400, WIDE), 0) + n * 400 == next_lane
        target += jnp.sum(jnp.where(here, part, 0.0), axis=0, keepdims=True)
    top = functools.reduce(jnp.maximum, tops)
    local_lse = top + jnp.log(sum(jnp.exp(t - top) * e for t, e in zip(tops, sums)))

    fin_s[...] = jnp.zeros_like(fin_s)
    for g in range(STEPS):
        for at, vec in ((g, local_lse), (2 + g, target)):
            fin_s[0, pl.ds(at, 1), :] = jnp.where(core == g, vec[:, LANE:], vec[:, :LANE])

    def merge(parts):
        high = functools.reduce(jnp.maximum, parts)
        scale_sum = sum(jnp.exp(part - high) for part in parts)
        return jnp.where(iota((SUB, LANE), 0) < 2, high + jnp.log(scale_sum), sum(parts))

    def fp_copy(k):
        return rcopy(fin_s.at[1], fin_p.at[plane], fp_s.at[0], fp_r.at[0], plane_dev(ahead(k)))

    def ff_copy(k):
        return rcopy(fin_s.at[2], fin_f.at[line], ff_s.at[0], ff_r.at[0], line_dev(k))

    down = rcopy(fin_s.at[0], fin_d.at[0], fd_s.at[0], fd_r.at[0], partner)
    back = rcopy(fin_s.at[3], fin_d.at[1], fd_s.at[0], fd_r.at[0], partner)

    @pl.when(core == 0)
    def _():
        down.start()
        back.wait_recv()
        down.wait_send()

    @pl.when(core == 1)
    def _():
        down.wait_recv()
        fin_s[1] = merge([fin_d[0], fin_s[0]])
        each_plane(lambda k: fp_copy(k).start())
        fin_p[plane] = fin_s[1]
        take(fin_p.at[FIFTEEN], fp_r.at[0])
        fin_s[2] = merge([fin_p[i] for i in range(SIDE)])
        for k in LINE_ORDER:
            ff_copy(k).start()
        fin_f[line] = fin_s[2]
        take(fin_f.at[THREE], ff_r.at[0])
        fin_s[3] = merge([fin_f[i] for i in range(LINE)])
        back.start()
        fin_d[1] = fin_s[3]
        take(fin_p.at[FIFTEEN], fp_s.at[0])
        take(fin_f.at[THREE], ff_s.at[0])
        back.wait_send()

    final = fin_d[1]
    lane_b = sequence_of(lane_q, lane_q >> 7)
    lp_lane = jnp.concatenate([final[2:3] - final[0:1], final[3:LINE] - final[1:2]], axis=1)
    for s in range(STEPS):
        col = jnp.sum(jnp.where((lane_b == sub_b) & (lane_s == s), lp_lane, 0.0), axis=1, keepdims=True)
        logp_ref[s:s + 1, :] = jnp.sum(jnp.where(diag, col, 0.0), axis=0, keepdims=True)

    for r in range(STEPS):
        take(send_d.at[r], sd_s.at[r])
        take(send_f.at[r, OTHERS], sf_s.at[r])
        take(recv_p.at[r, OTHERS], sp_s.at[r, 0])
        take(recv_p.at[r, FARTHER], sp_s.at[r, 1])
        take(recv_p.at[r, OTHERS], ap_s.at[r, 0])
        take(recv_p.at[r, FARTHER], ap_s.at[r, 1])
        take(ag.at[r, core, THREE], af_s.at[r])
        take(ag.at[r, core], ad_s.at[r])
    take(wext.at[THREE], wd_s.at[0])
    take(wext.at[pl.ds(0, 9)], wf_s.at[0])
    take(wext.at[pl.ds(0, 6)], wf_s.at[1])
    take(recv_q.at[PEERS], q_s.at[0])
    take(recv_a.at[PEERS], a_s.at[0])


def finish(logp_ref, kbuf, vbuf, logp_out, kout_hbm, vout_hbm, sems):
    copies = [pltpu.make_async_copy(kbuf, kout_hbm.at[0], sems.at[0]), pltpu.make_async_copy(vbuf, vout_hbm.at[0], sems.at[1])]
    for copy in copies:
        copy.start()
    logp_out[...] = logp_ref[...]
    for copy in copies:
        copy.wait()


def solution(mesh):
    def device_fn(tok_ids, next_ids, seq_lens, embed_loc, ln_gain, w_in_loc, w_out_loc, final_gain, k_loc, v_loc):
        half_dim = HEAD // 2
        inv_freq = np.power(np.float32(ROPE_BASE), -np.arange(half_dim, dtype=np.float32) / half_dim).reshape(1, half_dim)
        vmem = pl.BlockSpec(memory_space=pltpu.VMEM)
        hbm = pl.BlockSpec(memory_space=pltpu.HBM)
        dma = pltpu.SemaphoreType.DMA
        scratch = [
            pltpu.VMEM(tok_ids.shape, jnp.int32),
            pltpu.VMEM(next_ids.shape, jnp.int32),
            pltpu.SMEM(seq_lens.shape, jnp.int32),
            pltpu.VMEM((D,), BF16),
            pltpu.VMEM((D,), BF16),
            pltpu.VMEM((1, half_dim), F32),
            pltpu.VMEM((VPAD, D), BF16),
            pltpu.VMEM((276, D), BF16),
            pltpu.VMEM((WIDE, D), BF16),
            pltpu.VMEM((144, D), BF16),
            pltpu.VMEM((WIDE, D), BF16),
            pltpu.VMEM((ROWS, ATT_DEV, D), BF16),
            pltpu.VMEM((WIDE, 2560), BF16),
            pltpu.VMEM((WIDE, VPAD), BF16),
            pltpu.VMEM((STEPS, LANE, D), BF16),
            pltpu.VMEM((LANE, D), F32),
            pltpu.VMEM((STEPS, LANE, D), BF16),
            pltpu.VMEM((STEPS, LINE, LINE, SUB, D), BF16),
            pltpu.VMEM((STEPS, LINE, LINE, SUB, D), BF16),
            pltpu.VMEM((LINE, ROWS, D), F32),
            pltpu.VMEM((LINE, LANE, LANE), F32),
            pltpu.VMEM((FOLD, LANE), F32),
            pltpu.VMEM((STEPS, LINE, LANE, LANE), BF16),
            pltpu.VMEM((STEPS, SIDE, ROWS, LANE), BF16),
            pltpu.VMEM((ROWS, LANE), F32),
            pltpu.VMEM((ROWS, LANE), F32),
            pltpu.VMEM((STEPS, 2, LINE, LINE, LANE, LANE), BF16),
            pltpu.VMEM((4096, LANE), F32),
            pltpu.VMEM((WIDE, D), BF16),
            pltpu.VMEM((ROWS, D), BF16),
            pltpu.VMEM((LANE, LANE), F32),
            pltpu.VMEM((LANE, LANE), F32),
            pltpu.VMEM((ROWS, WIDE), BF16),
            pltpu.VMEM((ROWS, HEAD), F32),
            pltpu.VMEM((ROWS, LANE), F32),
            pltpu.VMEM((LINE, SUB, LANE), F32),
            pltpu.VMEM((LANE, LANE), F32),
            pltpu.VMEM((ROWS, FOLD), BF16),
            pltpu.VMEM((WIDE, LANE), BF16),
            pltpu.VMEM((LINE, SUB, LANE), F32),
            pltpu.VMEM((SIDE, SUB, LANE), F32),
            pltpu.VMEM((LINE, SUB, LANE), F32),
            pltpu.VMEM((STEPS, SUB, LANE), F32),
            dma((14,)),
            dma((STEPS,)), dma((5,)), dma((STEPS,)), dma((STEPS, LINE)), dma((STEPS, STEPS)), dma((STEPS, STEPS)),
            dma((STEPS, STEPS)), dma((STEPS, LINE)), dma((STEPS,)), dma((STEPS, LINE)), dma((STEPS,)), dma((STEPS,)),
            dma((1,)), dma((1,)), dma((STEPS,)), dma((STEPS,)),
            *[dma((1,)) for _ in range(10)],
        ]
        logp, k_done, v_done = pl.pallas_call(
            kernel,
            out_shape=(jax.ShapeDtypeStruct(tok_ids.shape, F32),
                       jax.ShapeDtypeStruct(k_loc.shape[1:], k_loc.dtype),
                       jax.ShapeDtypeStruct(v_loc.shape[1:], v_loc.dtype)),
            in_specs=[hbm] * 11,
            out_specs=(vmem, vmem, vmem),
            scratch_shapes=scratch,
            compiler_params=pltpu.CompilerParams(collective_id=0, has_side_effects=True, vmem_limit_bytes=48 * 2 ** 20),
        )(*[pltpu.with_memory_space_constraint(arr, pltpu.HBM) for arr in (tok_ids, next_ids, seq_lens, embed_loc, ln_gain, w_in_loc.T, w_out_loc, final_gain,
          k_loc, v_loc, inv_freq)])
        return pl.pallas_call(
            finish,
            out_shape=(jax.ShapeDtypeStruct(tok_ids.shape, F32),
                       jax.ShapeDtypeStruct(k_loc.shape, k_loc.dtype),
                       jax.ShapeDtypeStruct(v_loc.shape, v_loc.dtype)),
            in_specs=[vmem, vmem, vmem],
            out_specs=(vmem, pl.BlockSpec(memory_space=pl.ANY), pl.BlockSpec(memory_space=pl.ANY)),
            scratch_shapes=[dma((STEPS,))],
            compiler_params=pltpu.CompilerParams(vmem_limit_bytes=8 * 2 ** 20),
        )(logp, k_done, v_done)

    cache_spec = P('tp', None, None)
    return jax.shard_map(device_fn, mesh=mesh, in_specs=(P(), P(), P(), P('tp', None), P(), P(None, 'tp'), P('tp', None), P(), cache_spec, cache_spec), out_specs=(P(), cache_spec, cache_spec), check_vma=False)
```
